32 devices in a mesh: stream: 8 (over z, x), span: 4 (over y, core).
Axes of the slice: x: 2, y: 2, z: 4, core: 2. Of those that a mesh axis runs over, the one named last changes fastest.
Arguments:
- state: float32 [320, 8, 625], P('stream', 'span'), may hold values from -0.25 to 2.5, as said below
- direction: float32 [320, 8, 625], P('stream', 'span'), may hold values from -6 to 6
- metric: float32 [320, 8, 3], P('stream', 'span'), may hold values from 1 to 4
- face_source: int32 [320, 4], P('stream'), may hold values from -1 to 225, as said below
- send_rows: int32 [8, 2, 33], P('stream'), may hold values from 0 to 159, as said below
Outputs:
- residual: float32 [320, 8, 625], P('stream', 'span')
- basis_next: float32 [320, 8, 625], P('stream', 'span')
- krylov: float32 [3], replicated
The draws below stay inside these ranges and needn't reach their ends.
Inputs may be any that keep to these rules, and one draw needn't show every extreme that they name: `state`: conserved variables from density 0.75 to 1.25, flow-wise velocity 0.1 to 0.5, other velocities -0.2 to 0.2, pressure 0.5 to 0.9, so pressure and temperature are positive. `face_source`: the plane is a grid of columns of 32 cells, numbered column by column, partition d owning cells d * 40 to (d + 1) * 40 - 1 in a random local order; flow-wise faces wrap around. Every face neighbour lies in the same or an adjacent partition; -1 stands exactly on the lower face of the lowest and the upper face of the highest row; indices into received blocks point at used slots. `send_rows`: at most 33 faces per neighbouring pair, and some pair uses all 33; slots beyond a pair's count hold 0; the order of slots is the order in which the receiver's face_source refers to them.
All inputs are finite; a program needn't handle non-finite values.
Results may differ from the reference program's by a relative error of at most 0.0003.
Values sent between devices are 32-bit elements.
A program may use at most 128 MiB of HBM per device.

```python
import math
import jax
import jax.numpy as jnp
import numpy as np
from jax import lax

COLUMNS = 40
WALL_ROWS = 32
NODES = 125
VARS = 5
SLOTS = 33
PLANE = 320
LAYERS = 8
N_STREAM = 8


GAMMA_RATIO = 1.4


def draw_state(key, part):
    noise_shape = (PLANE, LAYERS, 5, NODES)
    noise = jnp.clip(0.4 * jax.random.normal(key, noise_shape, jnp.float32), -1.0, 1.0)
    density = 1.0 + 0.25 * noise[:, :, 0]
    flow_speed = 0.3 + 0.2 * noise[:, :, 1]
    normal_speed = 0.2 * noise[:, :, 2]
    span_speed = 0.2 * noise[:, :, 3]
    pressure = 0.7 + 0.2 * noise[:, :, 4]
    kinetic = 0.5 * density * (flow_speed * flow_speed + normal_speed * normal_speed + span_speed * span_speed)
    energy = pressure / (GAMMA_RATIO - 1.0) + kinetic
    stacked = jnp.stack([density, density * flow_speed, density * normal_speed, density * span_speed, energy], axis=2)
    return stacked.reshape(PLANE, LAYERS, 5 * NODES)


def mesh_tables(key):
    devices = N_STREAM
    cell_ids = jnp.arange(PLANE, dtype=jnp.int32)
    owner_part = cell_ids // COLUMNS
    position = cell_ids % COLUMNS
    part_keys = jax.random.split(jax.random.fold_in(key, 17), devices)
    orders = jax.vmap(lambda single: jax.random.permutation(single, COLUMNS))(part_keys).astype(jnp.int32)
    local_column = orders[owner_part, position]
    column_count = PLANE // WALL_ROWS
    flow_column = cell_ids // WALL_ROWS
    wall_row = cell_ids % WALL_ROWS
    neighbor = jnp.stack([(flow_column - 1) % column_count * WALL_ROWS + wall_row, (flow_column + 1) % column_count * WALL_ROWS + wall_row, cell_ids - 1, cell_ids + 1], axis=1)
    walled = jnp.stack([wall_row < 0, wall_row < 0, wall_row == 0, wall_row == WALL_ROWS - 1], axis=1)
    neighbor = jnp.where(walled, cell_ids[:, None], neighbor)
    other_owner = neighbor // COLUMNS
    face_ids = jnp.arange(4, dtype=jnp.int32)[None, :]
    to_left = jnp.logical_and(jnp.logical_not(walled), other_owner == (owner_part[:, None] - 1) % devices)
    to_right = jnp.logical_and(jnp.logical_not(walled), other_owner == (owner_part[:, None] + 1) % devices)

    def slots_of(flags):
        flat_flags = flags.reshape(devices, COLUMNS * 4).astype(jnp.int32)
        before = jnp.cumsum(flat_flags, axis=1) - flat_flags
        return before.reshape(PLANE, 4)
    left_slot = slots_of(to_left)
    right_slot = slots_of(to_right)
    own_index = local_column[:, None] * 4 + face_ids
    owners = jnp.broadcast_to(owner_part[:, None], (PLANE, 4))
    send_table = jnp.zeros((devices, 2, SLOTS), jnp.int32)
    send_table = send_table.at[owners, 0, jnp.where(to_left, left_slot, SLOTS)].set(own_index, mode='drop')
    send_table = send_table.at[owners, 1, jnp.where(to_right, right_slot, SLOTS)].set(own_index, mode='drop')
    partner_face = face_ids + 1 - 2 * (face_ids % 2)
    partner_local = local_column[neighbor] * 4 + partner_face
    from_right = COLUMNS * 4 + SLOTS + left_slot[neighbor, partner_face]
    from_left = COLUMNS * 4 + right_slot[neighbor, partner_face]
    source = jnp.where(to_right, from_right, jnp.where(to_left, from_left, partner_local))
    source = jnp.where(walled, -1, source).astype(jnp.int32)
    row_ids = owner_part * COLUMNS + local_column
    source_table = jnp.zeros((PLANE, 4), jnp.int32).at[row_ids].set(source)
    return (source_table, send_table)


def draw_face_source(key, part):
    return mesh_tables(key)[0]


def draw_send_rows(key, part):
    return mesh_tables(key)[1]


def levels(key, shape, pieces, least, high):
    factor_of, own = 1.0, jax.random.fold_in(key, 6)
    for axis_at, shards_of in pieces:
        draws = jnp.exp(jax.random.uniform(jax.random.fold_in(own, axis_at), (shards_of,), jnp.float32, least / len(pieces), high / len(pieces)))
        factor_of = factor_of * jnp.repeat(draws, shape[axis_at] // shards_of).reshape([-1 if axis == axis_at else 1 for axis in range(len(shape))])
    return factor_of


def bell_draw(key, extent, scale, limit, shards=(), held_as=jnp.bfloat16):
    values = scale * jax.random.normal(key, extent, jnp.float32)
    if shards:
        values = values * levels(key, extent, shards, -0.22, 0.18)
    return jnp.clip(values, -limit, limit).astype(held_as)


def setup_inputs(seed: int = 0) -> dict:
    arg_keys = jax.random.split(jax.random.key(seed), 6)
    return {
        "state": draw_state(jax.random.fold_in(arg_keys[5], 71), 0),
        "direction": bell_draw(arg_keys[1], (PLANE, LAYERS, NODES * VARS), 1.0, 6.0, ((0, 8), (1, 4)), jnp.float32),
        "metric": jnp.clip(jnp.exp(math.log(4.0) - 1.3862944 * jax.random.uniform(arg_keys[2], (PLANE, LAYERS, 3), jnp.float32) ** levels(arg_keys[2], (PLANE, LAYERS, 3), ((0, 8), (1, 4)), -0.2, 0.2)), 1.0, 4.0),
        "face_source": draw_face_source(jax.random.fold_in(arg_keys[5], 71), 0),
        "send_rows": draw_send_rows(jax.random.fold_in(arg_keys[5], 71), 0),
    }


GAMMA = 1.4
VISC = 0.01
COND = VISC * GAMMA / ((GAMMA - 1.0) * 0.72)
LIFT = 10.0
EINSUM_FORMS = ('ai,...ijk->...ajk', 'aj,...ijk->...iak', 'ak,...ijk->...ija')

def diff_table():
    spread = math.sqrt(3.0 / 7.0)
    points = np.array([-1.0, -spread, 0.0, spread, 1.0])
    weights = np.array([np.prod([points[row_at] - points[other] for other in range(5) if other != row_at]) for row_at in range(5)])
    matrix = np.zeros((5, 5))
    for row_at in range(5):
        for col_at in range(5):
            if row_at != col_at:
                matrix[row_at, col_at] = weights[row_at] / (weights[col_at] * (points[row_at] - points[col_at]))
        matrix[row_at, row_at] = np.sum([1.0 / (points[row_at] - points[other]) for other in range(5) if other != row_at])
    return matrix

def derivative(field, axis_pick):
    matrix = jnp.asarray(diff_table(), dtype=jnp.float32)
    return jnp.einsum(EINSUM_FORMS[axis_pick], matrix, field, precision=lax.Precision.HIGHEST)

def face_slice(volume, face_index):
    endpoint = 4 * (face_index % 2)
    if face_index < 2:
        return volume[..., endpoint, :, :]
    if face_index < 4:
        return volume[..., :, endpoint, :]
    return volume[..., :, :, endpoint]

def put_face(volume, face_index, values):
    endpoint = 4 * (face_index % 2)
    if face_index < 2:
        return volume.at[..., endpoint, :, :].add(values)
    if face_index < 4:
        return volume.at[..., :, endpoint, :].add(values)
    return volume.at[..., :, :, endpoint].add(values)

def primitive(components):
    density = components[0]
    velocity = [components[1] / density, components[2] / density, components[3] / density]
    kinetic = 0.5 * (components[1] * velocity[0] + components[2] * velocity[1] + components[3] * velocity[2])
    pressure = (GAMMA - 1.0) * (components[4] - kinetic)
    return (velocity, pressure, pressure / density)

def inviscid(components, axis_pick):
    velocity, pressure, temper = primitive(components)
    normal_speed = velocity[axis_pick]
    result = [components[1 + axis_pick]]
    for member in range(3):
        flux_term = components[1 + member] * normal_speed
        if member == axis_pick:
            flux_term = flux_term + pressure
        result.append(flux_term)
    result.append((components[4] + pressure) * normal_speed)
    return result

def viscous(components, gradients, axis_pick):
    velocity, pressure, temper = primitive(components)
    divergence = gradients[0][0] + gradients[1][1] + gradients[2][2]
    stresses = []
    for member in range(3):
        stress = gradients[axis_pick][member] + gradients[member][axis_pick]
        if member == axis_pick:
            stress = stress - 2.0 / 3.0 * divergence
        stresses.append(VISC * stress)
    energy = stresses[0] * velocity[0] + stresses[1] * velocity[1] + stresses[2] * velocity[2] + COND * gradients[axis_pick][3]
    return [jnp.zeros_like(energy)] + stresses + [energy]

def wave_square(components):
    velocity, pressure, temper = primitive(components)
    return velocity[0] * velocity[0] + velocity[1] * velocity[1] + velocity[2] * velocity[2] + GAMMA * temper

def lifted_gradient(volume, outside, scales):
    components = [volume[..., member, :, :, :] for member in range(5)]
    velocity, pressure, temper = primitive(components)
    fields = velocity + [temper]
    outer_fields = []
    for face_index in range(6):
        outer_parts = [outside[face_index][..., member, :, :] for member in range(5)]
        outer_velocity, outer_pressure, outer_temper = primitive(outer_parts)
        outer_fields.append(outer_velocity + [outer_temper])
    gradients = []
    for axis_pick in range(3):
        factor = scales[..., axis_pick][..., None, None, None]
        grad_row = []
        for field_index in range(4):
            accumulated = derivative(fields[field_index], axis_pick)
            for upper_side in range(2):
                face_index = 2 * axis_pick + upper_side
                normal_sign = 2.0 * upper_side - 1.0
                trace_jump = outer_fields[face_index][field_index] - face_slice(fields[field_index], face_index)
                accumulated = put_face(accumulated, face_index, 0.5 * LIFT * normal_sign * trace_jump)
            grad_row.append(factor * accumulated)
        gradients.append(grad_row)
    return gradients

def own_viscous_faces(volume, gradients):
    components = [volume[..., member, :, :, :] for member in range(5)]
    result = []
    for face_index in range(6):
        face_parts = [face_slice(piece, face_index) for piece in components]
        face_grads = [[face_slice(entry, face_index) for entry in grad_row] for grad_row in gradients]
        result.append(jnp.stack(viscous(face_parts, face_grads, face_index // 2), axis=-3))
    return result

def residual_terms(volume, outside, gradients, visc_outside, scales, walls):
    components = [volume[..., member, :, :, :] for member in range(5)]
    totals = [jnp.zeros_like(components[0]) for member in range(5)]
    for axis_pick in range(3):
        factor = scales[..., axis_pick][..., None, None, None]
        convect = inviscid(components, axis_pick)
        diffuse = viscous(components, gradients, axis_pick)
        accumulated = [derivative(convect[member] - diffuse[member], axis_pick) for member in range(5)]
        for upper_side in range(2):
            face_index = 2 * axis_pick + upper_side
            normal_sign = 2.0 * upper_side - 1.0
            inner_parts = [face_slice(piece, face_index) for piece in components]
            outer_parts = [outside[face_index][..., member, :, :] for member in range(5)]
            outer_flux = inviscid(outer_parts, axis_pick)
            speed = jnp.sqrt(0.5 * (wave_square(inner_parts) + wave_square(outer_parts)))
            for member in range(5):
                inner_visc = face_slice(diffuse[member], face_index)
                outer_visc = visc_outside[face_index][..., member, :, :]
                if walls[face_index] is not None:
                    outer_visc = jnp.where(walls[face_index], inner_visc, outer_visc)
                surface = normal_sign * 0.5 * (outer_flux[member] - face_slice(convect[member], face_index)) - 0.5 * speed * (outer_parts[member] - inner_parts[member]) - normal_sign * 0.5 * (outer_visc - inner_visc)
                accumulated[member] = put_face(accumulated[member], face_index, LIFT * surface)
        totals = [totals[member] + factor * accumulated[member] for member in range(5)]
    return jnp.stack(totals, axis=-4)

def wall_masks(face_source):
    masks = [None, None, None, None, None, None]
    for face_index in (2, 3):
        masks[face_index] = (face_source[:, face_index] < 0)[:, None, None, None]
    return masks

def mirrored(face_trace):
    flips = 2.0 * (jnp.arange(5) % 4 == 0).astype(jnp.float32) - 1.0
    return face_trace * flips[:, None, None]

def pack_faces(volume):
    lead_shape = volume.shape[:2] + (-1,)
    return jnp.stack([face_slice(volume, face_index).reshape(lead_shape) for face_index in range(6)], axis=1)

def stack_faces(face_list):
    lead_shape = face_list[0].shape[:2] + (-1,)
    return jnp.stack([entry.reshape(lead_shape) for entry in face_list], axis=1)

def send_buffers(table, send_rows):
    picked = jnp.take(table, send_rows.reshape(-1), axis=0)
    return picked.reshape((2, send_rows.shape[2]) + table.shape[1:])

def pick_outside(table, received, face_source):
    whole = jnp.concatenate([table, received[0], received[3]], axis=0)
    picked = jnp.take(whole, jnp.maximum(face_source, 0).reshape(-1), axis=0)
    return picked.reshape(face_source.shape + table.shape[1:])

def split_traces(outside, upper_half, trailing):
    half_width = outside[0].shape[-1] // 2
    offset = half_width * upper_half
    return [entry[..., offset:offset + half_width].reshape(entry.shape[:-1] + trailing) for entry in outside]

def with_walls(outside, own_volume, walls):
    result = []
    for face_index in range(6):
        face_trace = outside[face_index]
        if walls[face_index] is not None:
            face_trace = jnp.where(walls[face_index][..., None], mirrored(face_slice(own_volume, face_index)), face_trace)
        result.append(face_trace)
    return result

def plane_reference(own_faces, face_source, send_rows):
    devices = send_rows.shape[0]
    table = own_faces[:, :4].reshape((devices, -1) + own_faces.shape[2:])
    buffers = jax.vmap(send_buffers)(table, send_rows[:, None])
    received = jnp.stack([jnp.roll(buffers[:, 1], 1, axis=0), buffers[:, 0], buffers[:, 1], jnp.roll(buffers[:, 0], -1, axis=0)], axis=1)
    plane = jax.vmap(pick_outside)(table, received, face_source.reshape(devices, -1, 4))
    plane = plane.reshape((-1,) + plane.shape[2:])
    return [plane[:, 0], plane[:, 1], plane[:, 2], plane[:, 3]]

def reference(state, direction, metric, face_source, send_rows):
    element = (5, 5, 5, 5)
    primal = jnp.moveaxis(state.reshape((PLANE, LAYERS) + element), 1, 0)[:, :, None]
    tangent = jnp.moveaxis(direction.reshape((PLANE, LAYERS) + element), 1, 0)[:, :, None]
    scales = jnp.moveaxis(metric, 1, 0)[:, :, None]
    walls = wall_masks(face_source)
    lead_shape = (LAYERS, PLANE, 1, -1)
    bottoms = jnp.concatenate([face_slice(primal, 4).reshape(lead_shape), face_slice(tangent, 4).reshape(lead_shape)], axis=-1)
    tops = jnp.concatenate([face_slice(primal, 5).reshape(lead_shape), face_slice(tangent, 5).reshape(lead_shape)], axis=-1)
    below_states = jnp.roll(tops, 1, axis=0)
    above_states = jnp.roll(bottoms, -1, axis=0)

    def first_section(volume_p, volume_t, scales_layer, below, above):
        own_states = jnp.concatenate([pack_faces(volume_p), pack_faces(volume_t)], axis=-1)
        outside = plane_reference(own_states, face_source, send_rows) + [below, above]
        outside_p = with_walls(split_traces(outside, 0, (5, 5, 5)), volume_p, walls)
        outside_t = with_walls(split_traces(outside, 1, (5, 5, 5)), volume_t, walls)
        grad_p, grad_t = jax.jvp(lambda volume, outer_side: lifted_gradient(volume, outer_side, scales_layer), (volume_p, outside_p), (volume_t, outside_t))
        return (outside_p, outside_t, grad_p, grad_t)

    def visc_section(inputs):
        volume_p, volume_t, scales_layer, below, above = inputs
        outside_p, outside_t, grad_p, grad_t = first_section(volume_p, volume_t, scales_layer, below, above)
        visc_p, visc_t = jax.jvp(own_viscous_faces, (volume_p, grad_p), (volume_t, grad_t))
        return jnp.concatenate([stack_faces(visc_p), stack_faces(visc_t)], axis=-1)
    own_visc = lax.map(visc_section, (primal, tangent, scales, below_states, above_states))
    visc_below = jnp.roll(own_visc[:, :, 5], 1, axis=0)
    visc_above = jnp.roll(own_visc[:, :, 4], -1, axis=0)

    def final_section(inputs):
        volume_p, volume_t, scales_layer, below, above, visc_own, visc_low, visc_high = inputs
        outside_p, outside_t, grad_p, grad_t = first_section(volume_p, volume_t, scales_layer, below, above)
        visc_out = plane_reference(visc_own, face_source, send_rows) + [visc_low, visc_high]
        visc_p = split_traces(visc_out, 0, (5, 5, 5))
        visc_t = split_traces(visc_out, 1, (5, 5, 5))
        return jax.jvp(lambda volume, outer_side, gradients, visc_side: residual_terms(volume, outer_side, gradients, visc_side, scales_layer, walls), (volume_p, outside_p, grad_p, visc_p), (volume_t, outside_t, grad_t, visc_t))
    res_p, res_t = lax.map(final_section, (primal, tangent, scales, below_states, above_states, own_visc, visc_below, visc_above))
    residual = jnp.moveaxis(res_p[:, :, 0], 0, 1).reshape(state.shape)
    product = jnp.moveaxis(res_t[:, :, 0], 0, 1).reshape(state.shape)
    total = float(state.size)
    coefficient = jnp.sum(direction * product) / total
    remainder = product - coefficient * direction
    beta = jnp.sqrt(jnp.sum(remainder * remainder) / total)
    norm_value = jnp.sqrt(jnp.sum(residual * residual) / total)
    return (residual, remainder / beta, jnp.stack([coefficient, beta, norm_value]))
```

```python
import functools
import math

import jax
import jax.numpy as jnp
import numpy as np
from jax import lax
from jax.experimental import pallas as pl
from jax.experimental.pallas import tpu as pltpu
from jax.sharding import PartitionSpec as P

GAMMA = 1.4
VISC = 0.01
COND = VISC * GAMMA / ((GAMMA - 1.0) * 0.72)
LIFT = 10.0
MESH = pl.DeviceIdType.MESH
F32, BF16 = jnp.float32, jnp.bfloat16


def diff_table():
    spread = math.sqrt(3.0 / 7.0)
    points = np.array([-1.0, -spread, 0.0, spread, 1.0])
    weights = np.array(
        [np.prod([points[i] - points[j] for j in range(5) if j != i]) for i in range(5)]
    )
    matrix = np.zeros((5, 5))
    for i in range(5):
        for j in range(5):
            if i != j:
                matrix[i, j] = weights[i] / (weights[j] * (points[i] - points[j]))
        matrix[i, i] = np.sum([1.0 / (points[i] - points[j]) for j in range(5) if j != i])
    return matrix


def operators(layers):
    table = diff_table()
    eye = np.eye(5)
    kron = [
        np.einsum("ai,bj,ck->ijkabc", *[table if m == a else eye for m in range(3)]).reshape(125, 125)
        for a in range(3)
    ]
    node = np.arange(125).reshape(5, 5, 5)
    vw, fw, half = 128 * layers, 64 * layers, 32 * layers
    deriv = np.zeros((3, vw, vw), np.float32)
    pick = np.zeros((3, vw, fw), np.float32)
    for a in range(3):
        for l in range(layers):
            b = 128 * l
            deriv[a, b : b + 125, b : b + 125] = kron[a]
            for side in range(2):
                face = np.take(node, 4 * side, axis=a).reshape(-1)
                for m, at in enumerate(face):
                    pick[a, b + at, side * half + 32 * l + m] = 1.0
    high = deriv.astype(jnp.bfloat16)
    low = (deriv - high.astype(np.float32)).astype(jnp.bfloat16)
    lift = np.swapaxes(pick, 1, 2)
    return high, low, lift.astype(jnp.bfloat16)


def pieces(x, n):
    out = []
    for i in range(n):
        p = x.astype(BF16)
        out.append(p)
        if i + 1 < n:
            x = x - p.astype(F32)
    return out


def dot(a, b):
    return jnp.dot(a, b, preferred_element_type=F32)


def left(x, w, n):
    return sum(dot(p, w) for p in pieces(x, n)[::-1])


def right(w, x, n):
    return sum(dot(w, p) for p in pieces(x, n)[::-1])


def derive(x, high, low):
    a, b = pieces(x, 2)
    return dot(a, low) + dot(b, high) + dot(a, high)


def fields_of(u):
    inv = 1.0 / u[0]
    vel = [u[1] * inv, u[2] * inv, u[3] * inv]
    kinetic = 0.5 * (u[1] * vel[0] + u[2] * vel[1] + u[3] * vel[2])
    pressure = (GAMMA - 1.0) * (u[4] - kinetic)
    return vel, pressure, pressure * inv


def inviscid(u, a):
    vel, pressure, _ = fields_of(u)
    out = [u[1 + a]]
    for m in range(3):
        term = u[1 + m] * vel[a]
        out.append(term + pressure if m == a else term)
    out.append((u[4] + pressure) * vel[a])
    return out


def viscous(vel, q, a, divergence):
    stress = []
    for m in range(3):
        term = q[a][m] + q[m][a]
        if m == a:
            term = term - 2.0 / 3.0 * divergence
        stress.append(VISC * term)
    energy = stress[0] * vel[0] + stress[1] * vel[1] + stress[2] * vel[2] + COND * q[a][3]
    return stress + [energy]


def viscous_all(u, q):
    inv = 1.0 / u[0]
    vel = [u[1] * inv, u[2] * inv, u[3] * inv]
    divergence = q[0][0] + q[1][1] + q[2][2]
    return [viscous(vel, q, a, divergence) for a in range(3)]


def gradient_fields(u):
    vel, _, temper = fields_of(u)
    return vel + [temper]


def jump_fields(inner, outer):
    return [o - i for o, i in zip(gradient_fields(outer), gradient_fields(inner))]


def surface(inner, outer, sign, a):
    vi, pi, ti = fields_of(inner)
    vo, po, to = fields_of(outer)
    square = sum(v * v for v in vi) + GAMMA * ti + sum(v * v for v in vo) + GAMMA * to
    speed = jnp.sqrt(0.5 * square)
    fi, fo = inviscid(inner, a), inviscid(outer, a)
    return [
        (0.5 * LIFT) * (sign * (fo[m] - fi[m]) - speed * (outer[m] - inner[m])) for m in range(5)
    ]


def ratio(top, bottom):
    return jnp.where(bottom > 0.0, top / jnp.where(bottom > 0.0, bottom, 1.0), 0.0)


def kernel(
    ns, np_,
    x_hbm, d_hbm, metric_hbm, fs_hbm, sr_hbm, key_hbm, dh_hbm, dl_hbm, lift_hbm,
    res_ref, prod_ref, own_ref, table_ref,
    u, uf, of, w, jf, q, v, vf, ov, g, s, r, mv, mf,
    sb1, rb1, zs1, zr1, sb2, rb2, zs2, zr2, st, sta,
    x_ref, d_ref, metric_ref, fs_ref, sr_ref, keyrow_ref, dh_ref, dl_ref, lift_ref,
    xsend, xrecv, asend, arecv, loads,
):
    C, L = x_ref.shape[0], x_ref.shape[1]
    VW, FW, half = 128 * L, 64 * L, 32 * L
    SLOTS = sr_ref.shape[2]
    SP = -(-SLOTS // 8) * 8
    MAIN, REM = SLOTS // 8, SLOTS % 8
    OWN = 4 * C
    ms, mp = lax.axis_index("stream"), lax.axis_index("span")
    lower, upper = lax.rem(ms + ns - 1, ns), lax.rem(ms + 1, ns)
    below, above = lax.rem(mp + np_ - 1, np_), lax.rem(mp + 1, np_)

    inputs = [
        pltpu.make_async_copy(src, dst, loads.at[i])
        for i, (src, dst) in enumerate(
            [
                (x_hbm, x_ref), (d_hbm, d_ref), (key_hbm, keyrow_ref),
                (fs_hbm, fs_ref), (sr_hbm, sr_ref), (metric_hbm, metric_ref),
                (dh_hbm, dh_ref), (dl_hbm, dl_ref), (lift_hbm, lift_ref),
            ]
        )
    ]
    for copy in inputs:
        copy.start()

    def peer(k):
        a, b = divmod(k, np_)
        return lax.rem(ms + a, ns), lax.rem(mp + b, np_)

    everyone = ns * np_
    barrier = pltpu.get_barrier_semaphore()
    for k in range(1, everyone):
        pl.semaphore_signal(barrier, inc=1, device_id=peer(k), device_id_type=MESH)

    fl = lax.broadcasted_iota(jnp.int32, (1, FW), 1)
    vl = lax.broadcasted_iota(jnp.int32, (1, VW), 1)
    first = fl < half
    sign = jnp.where(first, -1.0, 1.0)
    flayer = lax.rem(fl, half) // 32
    fnode = lax.rem(fl, 32)

    fside = jnp.where(first, 0, 1)
    outer, inner = fnode // 5, lax.rem(fnode, 5)
    nodes = [
        jnp.broadcast_to(jnp.where(fnode < 25, at, 127), (C, FW))
        for at in (100 * fside + fnode, 25 * outer + 20 * fside + inner, 5 * fnode + 4 * fside)
    ]

    def trace(volume, a):
        value = None
        for l in range(L):
            part = jnp.take_along_axis(
                volume[:, 128 * l : 128 * (l + 1)], nodes[a], axis=1, mode="promise_in_bounds"
            )
            value = part if value is None else jnp.where(flayer == l, part, value)
        return value

    def roll(x, shift):
        shift = shift % FW
        return pltpu.roll(x, shift, 1) if shift else x

    di = lax.broadcasted_iota(jnp.int32, (C, C), 0)
    dj = lax.broadcasted_iota(jnp.int32, (C, C), 1)

    def column(row):
        return jnp.sum(jnp.where(di == dj, row, 0.0), axis=1, keepdims=True)

    for copy in inputs[:2]:
        copy.wait()

    for pt, ref in enumerate((x_ref, d_ref)):
        for l in range(L):
            for m in range(5):
                pad = 1.0 if pt == 0 and m % 4 == 0 else 0.0
                u[pt, m, :, 128 * l + 120 : 128 * (l + 1)] = jnp.full((C, 8), pad, F32)
                u[pt, m, :, 128 * l : 128 * l + 125] = ref[:, l, 125 * m : 125 * (m + 1)]
    for copy in inputs[2:6]:
        copy.wait()
    keyrow = keyrow_ref[...].astype(F32)
    source = [column(fs_ref[f : f + 1, :].astype(F32)) for f in range(4)]
    onehot = jnp.concatenate(
        [
            jnp.where(source[2 * a + side] == keyrow, 1.0, 0.0)
            for side in range(2)
            for a in range(2)
        ],
        axis=0,
    ).astype(BF16)
    hot_own, hot_recv = onehot[:, :OWN], onehot[:, OWN : OWN + 2 * SP]
    ri = lax.broadcasted_iota(jnp.int32, (SP, SLOTS), 0)
    li = lax.broadcasted_iota(jnp.int32, (SP, SLOTS), 1)
    send_hot = []
    for side in range(2):
        row = sr_ref[0, side : side + 1, :].astype(F32)
        wanted = jnp.sum(jnp.where(ri == li, row, 0.0), axis=1, keepdims=True)
        send_hot.append(jnp.where(wanted == keyrow[:, :OWN], 1.0, 0.0))
    send_hot = jnp.concatenate(send_hot, axis=0).astype(BF16)

    def swap(a, b):
        return (
            jnp.where(first, a, pltpu.roll(b, half, 1)),
            jnp.where(first, pltpu.roll(a, half, 1), b),
        )

    def exchange(faces, members, sb, rb, zs, zr, base):
        blocks = [[swap(faces(0, m, a), faces(1, m, a)) for m in range(members)] for a in range(3)]
        table = jnp.concatenate(
            [
                jnp.concatenate([blocks[a][m][side] for m in range(members)], axis=1)
                for side in range(2)
                for a in range(2)
            ],
            axis=0,
        )
        for m in range(0, members, 2):
            for side in range(2):
                value = blocks[2][m][side]
                if m + 1 < members:
                    other = roll(blocks[2][m + 1][side], 32 if side == 0 else -32)
                    value = jnp.where(flayer == (0 if side == 0 else L - 1), value, other)
                zs[side, :, FW * (m // 2) : FW * (m // 2 + 1)] = value
        zs_copies = [
            (zs.at[0], zr.at[1], (ms, below)),
            (zs.at[1], zr.at[0], (ms, above)),
        ]
        copies = []
        for i, (src, dst, to) in enumerate(zs_copies):
            copies.append(
                pltpu.make_async_remote_copy(
                    src_ref=src, dst_ref=dst, send_sem=xsend.at[base + i],
                    recv_sem=xrecv.at[base + i], device_id=to, device_id_type=MESH,
                )
            )
        table_pieces = pieces(table, 3)
        sent = sum(dot(send_hot, p) for p in table_pieces[::-1])
        return blocks, table_pieces, sent, copies

    def finish_send(sent, sb, rb, base):
        for m in range(4):
            value = sent[:, FW * m : FW * (m + 1)]
            if sent.shape[1] > 4 * FW:
                spare = roll(sent[:, 4 * FW :], 25 - 7 * m)
                value = jnp.where(fnode < 25, value, spare)
            for side in range(2):
                for b in range(MAIN):
                    at = side * SP + 8 * b
                    sb[side, 4 * b + m] = value[at : at + 8]
                for e in range(REM):
                    at, to = side * SP + 8 * MAIN + e, REM * m + e
                    sb[side, 4 * MAIN + to // 8, to % 8 : to % 8 + 1, :] = value[at : at + 1]
        out = []
        for i, (src, dst, to) in enumerate(
            [
                (sb.at[0], rb.at[1], (lower, mp)),
                (sb.at[1], rb.at[0], (upper, mp)),
            ]
        ):
            out.append(
                pltpu.make_async_remote_copy(
                    src_ref=src, dst_ref=dst, send_sem=xsend.at[base + 2 + i],
                    recv_sem=xrecv.at[base + 2 + i], device_id=to, device_id_type=MESH,
                )
            )
        return out

    def plane_outside(own, rb, members, put):
        row8 = lax.broadcasted_iota(jnp.int32, (8, 1), 0)
        rows = []
        for side in range(2):
            rows += [
                jnp.concatenate([rb[side, 4 * b + m] for m in range(4)], axis=1)
                for b in range(MAIN)
            ]
            if REM:
                parts = []
                for m in range(4):
                    part = jnp.zeros((8, FW), F32)
                    for e in range(REM):
                        to = REM * m + e
                        line = rb[side, 4 * MAIN + to // 8, to % 8 : to % 8 + 1, :]
                        part = jnp.where(row8 == e, line, part)
                    parts.append(part)
                rows.append(jnp.concatenate(parts, axis=1))
        received = jnp.concatenate(rows, axis=0)
        if members * FW > received.shape[1]:
            spare = jnp.zeros((2 * SP, FW), F32)
            for m in range(received.shape[1] // FW):
                part = roll(received[:, FW * m : FW * (m + 1)], 7 * m - 25)
                spare = jnp.where((fnode >= 7 * m) & (fnode < 7 * m + 7), part, spare)
            received = jnp.concatenate([received, spare], axis=1)
        got = own + right(hot_recv, received, 3)
        for a in range(2):
            for m in range(members):
                lanes = slice(FW * m, FW * (m + 1))
                lo = got[a * C : (a + 1) * C, lanes]
                hi = got[(2 + a) * C : (3 + a) * C, lanes]
                primal, tangent = swap(lo, hi)
                put(0, m, a, primal)
                put(1, m, a, tangent)

    def layer_outside(blocks, zr, members, put):
        for m in range(members):
            lanes = slice(FW * (m // 2), FW * (m // 2 + 1))
            step = 32 * (L - 1 if m % 2 == 0 else L - 2)
            lo = jnp.where(flayer == 0, roll(zr[0, :, lanes], -step), roll(blocks[2][m][1], 32))
            hi = jnp.where(flayer == L - 1, roll(zr[1, :, lanes], step), roll(blocks[2][m][0], -32))
            primal, tangent = swap(lo, hi)
            put(0, m, 2, primal)
            put(1, m, 2, tangent)

    for a in range(3):
        for pt in range(2):
            for m in range(5):
                uf[pt, m, a] = trace(u[pt, m], a)
    blocks1, table1, sent1, zcopies1 = exchange(
        lambda pt, m, a: uf[pt, m, a], 5, sb1, rb1, zs1, zr1, 0
    )
    pcopies1 = finish_send(sent1, sb1, rb1, 0)
    pl.semaphore_wait(barrier, everyone - 1)
    for copy in pcopies1 + zcopies1:
        copy.start()
    for a in range(3):
        wide = jnp.zeros((C, VW), F32)
        face = jnp.zeros((C, FW), F32)
        for l in range(L):
            value = column(metric_ref[a, l : l + 1, :])
            wide = jnp.where(vl // 128 == l, value, wide)
            face = jnp.where(flayer == l, value, face)
        mv[a] = wide
        mf[a] = face

    for copy in inputs[6:]:
        copy.wait()

    own1 = sum(dot(hot_own, p) for p in table1[::-1])

    @pl.loop(0, C // 8, unroll=True)
    def _(i):
        rows = pl.ds(pl.multiple_of(i * 8, 8), 8)
        primal = [u[0, m, rows, :] for m in range(5)]
        tangent = [u[1, m, rows, :] for m in range(5)]
        fp, ft = jax.jvp(gradient_fields, (primal,), (tangent,))
        for m in range(4):
            w[0, m, rows, :] = fp[m]
            w[1, m, rows, :] = ft[m]

    fields = w[...].reshape(8 * C, VW)
    for a in range(3):
        q[a] = derive(fields, dh_ref[a], dl_ref[a]).reshape(2, 4, C, VW)

    for copy in zcopies1 + pcopies1:
        copy.wait()
    low_wall = jnp.where(source[2] < 0.0, 1.0, 0.0)
    high_wall = jnp.where(source[3] < 0.0, 1.0, 0.0)
    wall = jnp.where(first, low_wall, high_wall) > 0.5

    def put1(pt, m, a, value):
        if a == 1:
            own = uf[pt, m, a]
            value = jnp.where(wall, own if m % 4 == 0 else -own, value)
        of[pt, m, a] = jnp.where(fnode < 25, value, uf[pt, m, a])

    plane_outside(own1, rb1, 5, put1)
    layer_outside(blocks1, zr1, 5, put1)

    for a in range(3):
        @pl.loop(0, C // 8, unroll=True)
        def _(i):
            rows = pl.ds(pl.multiple_of(i * 8, 8), 8)
            primal = ([uf[0, m, a, rows, :] for m in range(5)], [of[0, m, a, rows, :] for m in range(5)])
            tangent = ([uf[1, m, a, rows, :] for m in range(5)], [of[1, m, a, rows, :] for m in range(5)])
            jp, jt = jax.jvp(jump_fields, primal, tangent)
            for m in range(4):
                jf[a, 0, m, rows, :] = (0.5 * LIFT) * sign * jp[m]
                jf[a, 1, m, rows, :] = (0.5 * LIFT) * sign * jt[m]

        q[a] += left(jf[a].reshape(8 * C, FW), lift_ref[a], 2).reshape(2, 4, C, VW)

    @pl.loop(0, C // 8, unroll=True)
    def _(i):
        rows = pl.ds(pl.multiple_of(i * 8, 8), 8)
        scale = [mv[a, rows, :] for a in range(3)]
        states = [[u[pt, m, rows, :] for m in range(5)] for pt in range(2)]
        grads = [
            [[scale[a] * q[a, pt, m, rows, :] for m in range(4)] for a in range(3)]
            for pt in range(2)
        ]
        vp, vt = jax.jvp(viscous_all, (states[0], grads[0]), (states[1], grads[1]))
        for a in range(3):
            for m in range(4):
                v[a, 0, m, rows, :] = vp[a][m]
                v[a, 1, m, rows, :] = vt[a][m]

    for a in range(3):
        for pt in range(2):
            for m in range(4):
                vf[a, pt, m] = trace(v[a, pt, m], a)
    blocks2, table2, sent2, zcopies2 = exchange(
        lambda pt, m, a: vf[a, pt, m], 4, sb2, rb2, zs2, zr2, 4
    )
    pcopies2 = finish_send(sent2, sb2, rb2, 4)
    for copy in pcopies2 + zcopies2:
        copy.start()

    own2 = sum(dot(hot_own, p) for p in table2[::-1])

    @pl.loop(0, C // 8, unroll=True)
    def _(i):
        rows = pl.ds(pl.multiple_of(i * 8, 8), 8)
        states = [[u[pt, m, rows, :] for m in range(5)] for pt in range(2)]
        for a in range(3):
            scale = mv[a, rows, :]
            fluxes = jax.jvp(lambda x: inviscid(x, a), (states[0],), (states[1],))
            for pt in range(2):
                g[a, pt, 0, rows, :] = scale * fluxes[pt][0]
                for m in range(4):
                    g[a, pt, m + 1, rows, :] = scale * (fluxes[pt][m + 1] - v[a, pt, m, rows, :])

    for a in range(3):
        @pl.loop(0, C // 8, unroll=True)
        def _(i):
            rows = pl.ds(pl.multiple_of(i * 8, 8), 8)
            primal = ([uf[0, m, a, rows, :] for m in range(5)], [of[0, m, a, rows, :] for m in range(5)])
            tangent = ([uf[1, m, a, rows, :] for m in range(5)], [of[1, m, a, rows, :] for m in range(5)])
            sp, stt = jax.jvp(
                lambda inner, outer: surface(inner, outer, sign, a), primal, tangent
            )
            for m in range(5):
                s[a, 0, m, rows, :] = sp[m]
                s[a, 1, m, rows, :] = stt[m]

    total = None
    for a in range(3):
        part = derive(g[a].reshape(10 * C, VW), dh_ref[a], dl_ref[a])
        total = part if total is None else total + part
    r[...] = total.reshape(2, 5, C, VW)

    for copy in zcopies2 + pcopies2:
        copy.wait()

    def put2(pt, m, a, value):
        if a == 1:
            value = jnp.where(wall, vf[a, pt, m], value)
        ov[a, pt, m] = value

    plane_outside(own2, rb2, 4, put2)
    layer_outside(blocks2, zr2, 4, put2)
    lifted = None
    for a in range(3):
        for pt in range(2):
            s[a, pt, 0] = mf[a] * s[a, pt, 0]
            for m in range(4):
                jump = ov[a, pt, m] - vf[a, pt, m]
                s[a, pt, m + 1] = mf[a] * (s[a, pt, m + 1] - (0.5 * LIFT) * sign * jump)
        part = left(s[a].reshape(10 * C, FW), lift_ref[a], 2)
        lifted = part if lifted is None else lifted + part
    r[...] += lifted.reshape(2, 5, C, VW)

    def whole_sum(parts):
        acc = parts[0]
        for part in parts[1:]:
            acc = acc + part
        return jnp.sum(jnp.sum(acc, axis=0, keepdims=True), axis=1, keepdims=True)

    pd = whole_sum([r[1, m] * u[1, m] for m in range(5)])
    dd = whole_sum([u[1, m] * u[1, m] for m in range(5)])
    rs = whole_sum([r[0, m] * r[0, m] for m in range(5)])
    mine = ratio(pd, dd)
    rests = [r[1, m] - mine * u[1, m] for m in range(5)]
    rr = whole_sum([x * x for x in rests])
    rd = whole_sum([x * u[1, m] for m, x in enumerate(rests)])
    lane = lax.broadcasted_iota(jnp.int32, (1, 128), 1)
    row = jnp.zeros((1, 128), F32)
    for i, value in enumerate((pd, dd, rs, rr, rd)):
        row = jnp.where(lane == i, value, row)
    st[...] = row
    copies = [
        pltpu.make_async_remote_copy(
            src_ref=st, dst_ref=sta.at[k], send_sem=asend.at[k], recv_sem=arecv.at[k],
            device_id=peer(k), device_id_type=MESH,
        )
        for k in range(1, everyone)
    ]
    for copy in copies:
        copy.start()
    sta[0] = st[...]
    own_ref[...] = d_ref[...]
    for pt, part in enumerate((res_ref, prod_ref)):
        for l in range(L):
            for m in range(5):
                part[:, l, 125 * m : 125 * (m + 1)] = r[pt, m, :, 128 * l : 128 * l + 125]
    for copy in copies:
        copy.wait()
    table_ref[...] = sta[...].reshape(everyone, 128)


def finish(total_count, res, prod, d, table_ref, res_hbm, basis_hbm, kry_ref, basis, sems):
    first = pltpu.make_async_copy(res, res_hbm, sems.at[0])
    first.start()
    lane = lax.broadcasted_iota(jnp.int32, (1, 128), 1)
    table = table_ref[...]
    pd, dd, rs, rr, rd = [
        jnp.sum(jnp.where(lane == i, table, 0.0), axis=1, keepdims=True) for i in range(5)
    ]
    coefficient = jnp.sum(pd, axis=0, keepdims=True) * (1.0 / total_count)
    shift = ratio(pd, dd) - coefficient
    rr = jnp.sum(rr + 2.0 * shift * rd + shift * shift * dd, axis=0, keepdims=True)
    rs = jnp.sum(rs, axis=0, keepdims=True)
    beta = jnp.sqrt(rr * (1.0 / total_count))
    norm = jnp.sqrt(rs * (1.0 / total_count))
    row = jnp.where(lane == 0, coefficient, jnp.where(lane == 1, beta, norm))
    kry_ref[...] = row[0, :3]
    c, inv = coefficient, 1.0 / beta
    basis[...] = (prod[...] - c[:, :, None] * d[...]) * inv[:, :, None]
    second = pltpu.make_async_copy(basis, basis_hbm, sems.at[1])
    second.start()
    first.wait()
    second.wait()


def local(ns, np_, state, direction, metric, face_source, send_rows):
    C, L, width = state.shape
    slots = send_rows.shape[2]
    SP = -(-slots // 8) * 8
    VW, FW = 128 * L, 64 * L
    own = 4 * C
    keys = np.full((1, own + 2 * SP), -7, np.int32)
    side, rest = np.divmod(np.arange(own), 2 * C)
    keys[0, :own] = 4 * (rest % C) + 2 * (rest // C) + side
    keys[0, own : own + slots] = own + np.arange(slots)
    keys[0, own + SP : own + SP + slots] = own + slots + np.arange(slots)
    tiles = 4 * (slots // 8) + -(-4 * (slots % 8) // 8)
    high, low, lift = operators(L)
    operands = (
        state, direction, jnp.transpose(metric, (2, 1, 0)), face_source.T, send_rows,
        *[jnp.asarray(x) for x in (keys, high, low, lift)],
    )
    operands = [pltpu.with_memory_space_constraint(x, pltpu.HBM) for x in operands]
    vmem = lambda *shape: pltpu.VMEM(shape, F32)
    dma = lambda n: pltpu.SemaphoreType.DMA((n,))
    spec = pl.BlockSpec(memory_space=pltpu.VMEM)
    parts, product, own, table = pl.pallas_call(
        functools.partial(kernel, ns, np_),
        out_shape=(
            *[jax.ShapeDtypeStruct(state.shape, F32)] * 3,
            jax.ShapeDtypeStruct((ns * np_, 128), F32),
        ),
        in_specs=[pl.BlockSpec(memory_space=pltpu.HBM)] * 9,
        out_specs=(spec,) * 4,
        scratch_shapes=[
            vmem(2, 5, C, VW), vmem(2, 5, 3, C, FW), vmem(2, 5, 3, C, FW),
            vmem(2, 4, C, VW), vmem(3, 2, 4, C, FW), vmem(3, 2, 4, C, VW),
            vmem(3, 2, 4, C, VW), vmem(3, 2, 4, C, FW), vmem(3, 2, 4, C, FW),
            vmem(3, 2, 5, C, VW), vmem(3, 2, 5, C, FW), vmem(2, 5, C, VW),
            vmem(3, C, VW), vmem(3, C, FW),
            vmem(2, tiles, 8, FW), vmem(2, tiles, 8, FW), vmem(2, C, 3 * FW), vmem(2, C, 3 * FW),
            vmem(2, tiles, 8, FW), vmem(2, tiles, 8, FW), vmem(2, C, 2 * FW), vmem(2, C, 2 * FW),
            vmem(1, 128), vmem(ns * np_, 1, 128),
            *[pltpu.VMEM(x.shape, x.dtype) for x in operands],
            dma(8), dma(8), dma(ns * np_), dma(ns * np_), dma(9),
        ],
        compiler_params=pltpu.CompilerParams(
            collective_id=0, has_side_effects=True, vmem_limit_bytes=40 * 1024 * 1024
        ),
        name="navier",
    )(*operands)
    hbm = pl.BlockSpec(memory_space=pltpu.HBM)
    return pl.pallas_call(
        functools.partial(finish, float(state.size * ns * np_)),
        out_shape=(
            jax.ShapeDtypeStruct(state.shape, F32),
            jax.ShapeDtypeStruct(state.shape, F32),
            jax.ShapeDtypeStruct((3,), F32),
        ),
        in_specs=[spec] * 4,
        out_specs=(hbm, hbm, spec),
        scratch_shapes=[vmem(C, L, width), dma(2)],
        compiler_params=pltpu.CompilerParams(vmem_limit_bytes=16 * 1024 * 1024),
        name="finish",
    )(parts, product, own, table)


def solution(mesh):
    return jax.shard_map(
        functools.partial(local, mesh.shape["stream"], mesh.shape["span"]),
        mesh=mesh,
        in_specs=(
            P("stream", "span", None),
            P("stream", "span", None),
            P("stream", "span", None),
            P("stream", None),
            P("stream", None, None),
        ),
        out_specs=(P("stream", "span", None), P("stream", "span", None), P()),
        check_vma=False,
    )
```

```python
import functools
import math

import jax
import jax.numpy as jnp
import numpy as np
from jax import lax
from jax.experimental import pallas as pl
from jax.experimental.pallas import tpu as pltpu
from jax.sharding import PartitionSpec as P

GAMMA = 1.4
VISC = 0.01
COND = VISC * GAMMA / ((GAMMA - 1.0) * 0.72)
LIFT = 10.0
MESH = pl.DeviceIdType.MESH
F32, BF16 = jnp.float32, jnp.bfloat16


def diff_table():
    spread = math.sqrt(3.0 / 7.0)
    points = np.array([-1.0, -spread, 0.0, spread, 1.0])
    weights = np.array(
        [np.prod([points[i] - points[j] for j in range(5) if j != i]) for i in range(5)]
    )
    matrix = np.zeros((5, 5))
    for i in range(5):
        for j in range(5):
            if i != j:
                matrix[i, j] = weights[i] / (weights[j] * (points[i] - points[j]))
        matrix[i, i] = np.sum([1.0 / (points[i] - points[j]) for j in range(5) if j != i])
    return matrix


def operators(layers):
    table = diff_table()
    eye = np.eye(5)
    kron = [
        np.einsum("ai,bj,ck->ijkabc", *[table if m == a else eye for m in range(3)]).reshape(125, 125)
        for a in range(3)
    ]
    node = np.arange(125).reshape(5, 5, 5)
    vw, fw, half = 128 * layers, 64 * layers, 32 * layers
    deriv = np.zeros((3, vw, vw), np.float32)
    pick = np.zeros((3, vw, fw), np.float32)
    for a in range(3):
        for l in range(layers):
            b = 128 * l
            deriv[a, b : b + 125, b : b + 125] = kron[a]
            for side in range(2):
                face = np.take(node, 4 * side, axis=a).reshape(-1)
                for m, at in enumerate(face):
                    pick[a, b + at, side * half + 32 * l + m] = 1.0
    high = deriv.astype(jnp.bfloat16)
    low = (deriv - high.astype(np.float32)).astype(jnp.bfloat16)
    lift = np.swapaxes(pick, 1, 2).astype(jnp.bfloat16)
    return np.concatenate([low, high, lift], axis=1)


def pieces(x, n):
    out = []
    for i in range(n):
        p = x.astype(BF16)
        out.append(p)
        if i + 1 < n:
            x = x - p.astype(F32)
    return out


def dot(a, b):
    return jnp.dot(a, b, preferred_element_type=F32)


def fields_of(u):
    inv = 1.0 / u[0]
    vel = [u[1] * inv, u[2] * inv, u[3] * inv]
    kinetic = 0.5 * (u[1] * vel[0] + u[2] * vel[1] + u[3] * vel[2])
    pressure = (GAMMA - 1.0) * (u[4] - kinetic)
    return vel, pressure, pressure * inv


def inviscid(u, a):
    vel, pressure, _ = fields_of(u)
    out = [u[1 + a]]
    for m in range(3):
        term = u[1 + m] * vel[a]
        out.append(term + pressure if m == a else term)
    out.append((u[4] + pressure) * vel[a])
    return out


def viscous(vel, q, a, divergence):
    stress = []
    for m in range(3):
        term = q[a][m] + q[m][a]
        if m == a:
            term = term - 2.0 / 3.0 * divergence
        stress.append(VISC * term)
    energy = stress[0] * vel[0] + stress[1] * vel[1] + stress[2] * vel[2] + COND * q[a][3]
    return stress + [energy]


def viscous_all(u, q):
    inv = 1.0 / u[0]
    vel = [u[1] * inv, u[2] * inv, u[3] * inv]
    divergence = q[0][0] + q[1][1] + q[2][2]
    return [viscous(vel, q, a, divergence) for a in range(3)]


def viscous_at(u, q, a):
    inv = 1.0 / u[0]
    vel = [u[1] * inv, u[2] * inv, u[3] * inv]
    return viscous(vel, q, a, q[0][0] + q[1][1] + q[2][2])


def gradient_fields(u):
    vel, _, temper = fields_of(u)
    return vel + [temper]


def jump_fields(inner, outer):
    return [o - i for o, i in zip(gradient_fields(outer), gradient_fields(inner))]


def surface(inner, outer, sign, a):
    vi, pi, ti = fields_of(inner)
    vo, po, to = fields_of(outer)
    square = sum(v * v for v in vi) + GAMMA * ti + sum(v * v for v in vo) + GAMMA * to
    speed = jnp.sqrt(0.5 * square)
    fi, fo = inviscid(inner, a), inviscid(outer, a)
    return [
        (0.5 * LIFT) * (sign * (fo[m] - fi[m]) - speed * (outer[m] - inner[m])) for m in range(5)
    ]


def ratio(top, bottom):
    return jnp.where(bottom > 0.0, top / jnp.where(bottom > 0.0, bottom, 1.0), 0.0)


def needed(a):
    return [(a, f) for f in range(4)] + [x for b in range(3) if b != a for x in ((b, a), (b, b))]


def kernel(
    ns, np_,
    x_hbm, d_hbm, metric_hbm, fs_hbm, sr_hbm, key_hbm, ops_hbm,
    res_ref, prod_ref, own_ref, table_ref,
    u, uf, of, w, jf, q, qf, vf, g, s, r, mv, mf,
    sb1, rb1, zs1, zr1, sb2, rb2, zs2, zr2, st, sta,
    xd, metric_ref, fs_ref, sr_ref, key_ref, ops_ref,
    xsend, xrecv, stsem, loads,
):
    C, L = xd.shape[1], xd.shape[2]
    VW, FW, half = 128 * L, 64 * L, 32 * L
    SLOTS = sr_ref.shape[2]
    SP = -(-SLOTS // 8) * 8
    MAIN, REM = SLOTS // 8, SLOTS % 8
    OWN = 4 * C
    ms, mp = lax.axis_index("stream"), lax.axis_index("span")
    lower, upper = lax.rem(ms + ns - 1, ns), lax.rem(ms + 1, ns)
    below, above = lax.rem(mp + np_ - 1, np_), lax.rem(mp + 1, np_)

    inputs = [
        pltpu.make_async_copy(src, dst, loads.at[i])
        for src, dst, i in [
            (x_hbm, xd.at[0], 0), (d_hbm, xd.at[1], 0), (key_hbm, key_ref, 1), (fs_hbm, fs_ref, 2),
            (sr_hbm, sr_ref, 3), (metric_hbm, metric_ref, 4), (ops_hbm, ops_ref, 5),
        ]
    ]
    for copy in inputs:
        copy.start()

    def peer(k):
        a, b = divmod(k, np_)
        return lax.rem(ms + a, ns), lax.rem(mp + b, np_)

    everyone = ns * np_
    barrier = pltpu.get_barrier_semaphore()
    for k in range(1, everyone):
        pl.semaphore_signal(barrier, inc=1, device_id=peer(k), device_id_type=MESH)

    fl = lax.broadcasted_iota(jnp.int32, (1, FW), 1)
    vl = lax.broadcasted_iota(jnp.int32, (1, VW), 1)
    first = fl < half
    sign = jnp.where(first, -1.0, 1.0)
    flayer = lax.rem(fl, half) // 32
    fnode = lax.rem(fl, 32)
    fside = jnp.where(first, 0, 1)
    major, minor = fnode // 5, lax.rem(fnode, 5)
    nodes = [
        jnp.where(fnode < 25, at, 127)
        for at in (100 * fside + fnode, 25 * major + 20 * fside + minor, 5 * fnode + 4 * fside)
    ]

    def pull(x, at):
        return jnp.take_along_axis(
            x, jnp.broadcast_to(at, x.shape), axis=1, mode="promise_in_bounds"
        )

    def trace(volume, a):
        value = None
        for l in range(L):
            part = pull(volume[:, 128 * l : 128 * (l + 1)], nodes[a])
            value = part if value is None else jnp.where(flayer == l, part, value)
        return value

    def edge(a, b):
        at = dict(zip([x for x in range(3) if x != a], (major, minor)))
        at[a] = 4 * fside
        one, two = [x for x in range(3) if x != b]
        there = (lax.rem(at[b], 4) == 0) & (fnode < 25)
        lane = half * (at[b] // 4) + 32 * flayer + 5 * at[one] + at[two]
        return there, jnp.where(there, lane, 0)

    edges = {(a, b): edge(a, b) for a in range(3) for b in range(3) if a != b}

    def roll(x, shift):
        shift = shift % FW
        return pltpu.roll(x, shift, 1) if shift else x

    di = lax.broadcasted_iota(jnp.int32, (C, C), 0)
    dj = lax.broadcasted_iota(jnp.int32, (C, C), 1)

    def column(row):
        return jnp.sum(jnp.where(di == dj, row, 0.0), axis=1, keepdims=True)

    def blocks_of(body):
        @pl.loop(0, C // 8, unroll=True)
        def _(i):
            body(pl.ds(pl.multiple_of(i * 8, 8), 8))

    def lift(axes, values):
        halves, table = [], []
        for a, value in zip(axes, values):
            halves += pieces(value, 2)
            table += [ops_ref[a, 2 * VW :]] * 2
        return dot(jnp.concatenate(halves, axis=1), jnp.concatenate(table, axis=0))

    def derive(axes, values):
        halves, table = [], []
        for a, value in zip(axes, values):
            high, low = pieces(value, 2)
            halves += [high, low, high]
            table += [ops_ref[a, : 2 * VW], ops_ref[a, VW : 2 * VW]]
        return dot(jnp.concatenate(halves, axis=1), jnp.concatenate(table, axis=0))

    def choose(hot, x):
        return dot(hot, jnp.concatenate(pieces(x, 3)[::-1], axis=0))

    def swap(a, b):
        return (
            jnp.where(first, a, pltpu.roll(b, half, 1)),
            jnp.where(first, pltpu.roll(a, half, 1), b),
        )

    def landed(ref, sem):
        pltpu.make_async_copy(ref, ref, sem).wait()

    def remote(pairs, base):
        for src, dst, to in pairs:
            pltpu.make_async_remote_copy(
                src_ref=src, dst_ref=dst, send_sem=xsend.at[base],
                recv_sem=xrecv.at[base], device_id=to, device_id_type=MESH,
            ).start()

    def arrived(source, target, base):
        landed(target, xrecv.at[base])
        landed(source, xsend.at[base])

    def plane_pack(faces, members, sb):
        blocks = [[swap(faces(0, m, a), faces(1, m, a)) for m in range(members)] for a in range(2)]
        table = jnp.concatenate(
            [
                jnp.concatenate([blocks[a][m][side] for m in range(members)], axis=1)
                for side in range(2)
                for a in range(2)
            ],
            axis=0,
        )
        sent = choose(send_hot, table)
        for m in range(4):
            value = sent[:, FW * m : FW * (m + 1)]
            if members > 4:
                spare = roll(sent[:, 4 * FW :], 25 - 7 * m)
                value = jnp.where(fnode < 25, value, spare)
            for side in range(2):
                for b in range(MAIN):
                    at = side * SP + 8 * b
                    sb[side, 4 * b + m] = value[at : at + 8]
                for e in range(REM):
                    at, to = side * SP + 8 * MAIN + e, REM * m + e
                    sb[side, 4 * MAIN + to // 8, to % 8 : to % 8 + 1, :] = value[at : at + 1]
        return table

    def plane_send(sb, rb, base):
        remote([(sb.at[0], rb.at[1], (lower, mp)), (sb.at[1], rb.at[0], (upper, mp))], base)

    def layer_send(faces, members, zs, zr, base):
        blocks = [swap(faces(0, m, 2), faces(1, m, 2)) for m in range(members)]
        for m in range(0, members, 2):
            for side in range(2):
                value = blocks[m][side]
                if m + 1 < members:
                    other = roll(blocks[m + 1][side], 32 if side == 0 else -32)
                    value = jnp.where(flayer == (0 if side == 0 else L - 1), value, other)
                zs[side, :, FW * (m // 2) : FW * (m // 2 + 1)] = value
        remote([(zs.at[0], zr.at[1], (ms, below)), (zs.at[1], zr.at[0], (ms, above))], base)
        return blocks

    def plane_outside(own, rb, members, put):
        row8 = lax.broadcasted_iota(jnp.int32, (8, 1), 0)
        rows = []
        for side in range(2):
            rows += [
                jnp.concatenate([rb[side, 4 * b + m] for m in range(4)], axis=1)
                for b in range(MAIN)
            ]
            if REM:
                parts = []
                for m in range(4):
                    part = jnp.zeros((8, FW), F32)
                    for e in range(REM):
                        to = REM * m + e
                        line = rb[side, 4 * MAIN + to // 8, to % 8 : to % 8 + 1, :]
                        part = jnp.where(row8 == e, line, part)
                    parts.append(part)
                rows.append(jnp.concatenate(parts, axis=1))
        received = jnp.concatenate(rows, axis=0)
        if members * FW > received.shape[1]:
            spare = jnp.zeros((2 * SP, FW), F32)
            for m in range(received.shape[1] // FW):
                part = roll(received[:, FW * m : FW * (m + 1)], 7 * m - 25)
                spare = jnp.where((fnode >= 7 * m) & (fnode < 7 * m + 7), part, spare)
            received = jnp.concatenate([received, spare], axis=1)
        got = own + choose(hot_recv, received)
        for a in range(2):
            for m in range(members):
                lanes = slice(FW * m, FW * (m + 1))
                lo = got[a * C : (a + 1) * C, lanes]
                hi = got[(2 + a) * C : (3 + a) * C, lanes]
                primal, tangent = swap(lo, hi)
                put(0, m, a, primal)
                put(1, m, a, tangent)

    def layer_outside(blocks, zr, members, put):
        for m in range(members):
            lanes = slice(FW * (m // 2), FW * (m // 2 + 1))
            step = 32 * (L - 1 if m % 2 == 0 else L - 2)
            lo = jnp.where(flayer == 0, roll(zr[0, :, lanes], -step), roll(blocks[m][1], 32))
            hi = jnp.where(flayer == L - 1, roll(zr[1, :, lanes], step), roll(blocks[m][0], -32))
            primal, tangent = swap(lo, hi)
            put(0, m, 2, primal)
            put(1, m, 2, tangent)

    landed(xd, loads.at[0])
    for pt in range(2):
        for l in range(L):
            for m in range(5):
                pad = 1.0 if pt == 0 and m % 4 == 0 else 0.0
                u[pt, m, :, 128 * l + 120 : 128 * (l + 1)] = jnp.full((C, 8), pad, F32)
                u[pt, m, :, 128 * l : 128 * l + 125] = xd[pt, :, l, 125 * m : 125 * (m + 1)]
    for copy in inputs[2:6]:
        copy.wait()
    own_keys, recv_keys = key_ref[0:1, : 3 * OWN], key_ref[1:2, : 6 * SP]
    source = [column(fs_ref[f : f + 1, :].astype(F32)) for f in range(4)]

    def hot(keys):
        rows = [jnp.where(source[2 * a + side] == keys, 1.0, 0.0) for side in range(2) for a in range(2)]
        return jnp.concatenate(rows, axis=0).astype(BF16)

    hot_own, hot_recv = hot(own_keys), hot(recv_keys)
    ri = lax.broadcasted_iota(jnp.int32, (SP, SLOTS), 0)
    li = lax.broadcasted_iota(jnp.int32, (SP, SLOTS), 1)
    send_hot = []
    for side in range(2):
        row = sr_ref[0, side : side + 1, :].astype(F32)
        wanted = jnp.sum(jnp.where(ri == li, row, 0.0), axis=1, keepdims=True)
        send_hot.append(jnp.where(wanted == own_keys, 1.0, 0.0))
    send_hot = jnp.concatenate(send_hot, axis=0).astype(BF16)

    def state_faces(a):
        for pt in range(2):
            for m in range(5):
                uf[pt, m, a] = trace(u[pt, m], a)

    state_faces(0)
    state_faces(1)
    table1 = plane_pack(lambda pt, m, a: uf[pt, m, a], 5, sb1)
    pl.semaphore_wait(barrier, everyone - 1)
    plane_send(sb1, rb1, 0)
    state_faces(2)
    blocks1 = layer_send(lambda pt, m, a: uf[pt, m, a], 5, zs1, zr1, 1)

    for a in range(3):
        wide = jnp.zeros((C, VW), F32)
        face = jnp.zeros((C, FW), F32)
        for l in range(L):
            value = column(metric_ref[a, l : l + 1, :])
            wide = jnp.where(vl // 128 == l, value, wide)
            face = jnp.where(flayer == l, value, face)
        mv[a] = wide
        mf[a] = face

    def gradients(rows):
        primal = [u[0, m, rows, :] for m in range(5)]
        tangent = [u[1, m, rows, :] for m in range(5)]
        fp, ft = jax.jvp(gradient_fields, (primal,), (tangent,))
        for m in range(4):
            w[0, m, rows, :] = fp[m]
            w[1, m, rows, :] = ft[m]

    blocks_of(gradients)
    inputs[6].wait()
    own1 = choose(hot_own, table1)
    fields = w[...].reshape(8 * C, VW)
    for a in range(3):
        q[a] = derive([a], [fields]).reshape(2, 4, C, VW)
    for a in range(3):
        for pt in range(2):
            for n, (b, f) in enumerate(needed(a)):
                qf[a, pt, n] = trace(q[b, pt, f], a)

    low_wall = jnp.where(source[2] < 0.0, 1.0, 0.0)
    high_wall = jnp.where(source[3] < 0.0, 1.0, 0.0)
    wall = jnp.where(first, low_wall, high_wall) > 0.5

    def put1(pt, m, a, value):
        if a == 1:
            own = uf[pt, m, a]
            value = jnp.where(wall, own if m % 4 == 0 else -own, value)
        of[pt, m, a] = jnp.where(fnode < 25, value, uf[pt, m, a])

    def jumps(a):
        def body(rows):
            primal = ([uf[0, m, a, rows, :] for m in range(5)], [of[0, m, a, rows, :] for m in range(5)])
            tangent = ([uf[1, m, a, rows, :] for m in range(5)], [of[1, m, a, rows, :] for m in range(5)])
            jp, jt = jax.jvp(jump_fields, primal, tangent)
            for m in range(4):
                jf[a, 0, m, rows, :] = (0.5 * LIFT) * sign * jp[m]
                jf[a, 1, m, rows, :] = (0.5 * LIFT) * sign * jt[m]

        blocks_of(body)

    def edge_jumps(a, b):
        there, lane = edges[a, b]
        for n, (other, f) in enumerate(needed(a)):
            if other == b:
                for pt in range(2):
                    qf[a, pt, n] += jnp.where(there, pull(jf[b, pt, f], lane), 0.0)

    arrived(zs1, zr1, 1)
    layer_outside(blocks1, zr1, 5, put1)
    jumps(2)
    edge_jumps(0, 2)
    edge_jumps(1, 2)
    arrived(sb1, rb1, 0)
    plane_outside(own1, rb1, 5, put1)
    jumps(0)
    jumps(1)
    edge_jumps(0, 1)
    edge_jumps(1, 0)

    def face_viscous(a):
        def body(rows):
            states = [[uf[pt, m, a, rows, :] for m in range(5)] for pt in range(2)]
            grads = []
            for pt in range(2):
                grad = [[None] * 4 for _ in range(3)]
                for n, (b, f) in enumerate(needed(a)):
                    value = qf[a, pt, n, rows, :]
                    if b == a:
                        value = value + jf[a, pt, f, rows, :]
                    grad[b][f] = mf[b, rows, :] * value
                grads.append(grad)
            vp, vt = jax.jvp(
                lambda x, y: viscous_at(x, y, a), (states[0], grads[0]), (states[1], grads[1])
            )
            for m in range(4):
                vf[a, 0, m, rows, :] = vp[m]
                vf[a, 1, m, rows, :] = vt[m]

        blocks_of(body)

    face_viscous(0)
    face_viscous(1)
    table2 = plane_pack(lambda pt, m, a: vf[a, pt, m], 4, sb2)
    plane_send(sb2, rb2, 2)
    edge_jumps(2, 0)
    edge_jumps(2, 1)
    face_viscous(2)
    blocks2 = layer_send(lambda pt, m, a: vf[a, pt, m], 4, zs2, zr2, 3)

    own2 = choose(hot_own, table2)
    for a in range(3):
        q[a] += lift([a], [jf[a].reshape(8 * C, FW)]).reshape(2, 4, C, VW)

    def fluxes(rows):
        scale = [mv[a, rows, :] for a in range(3)]
        states = [[u[pt, m, rows, :] for m in range(5)] for pt in range(2)]
        grads = [
            [[scale[a] * q[a, pt, m, rows, :] for m in range(4)] for a in range(3)]
            for pt in range(2)
        ]
        visc = jax.jvp(viscous_all, (states[0], grads[0]), (states[1], grads[1]))
        for a in range(3):
            euler = jax.jvp(lambda x: inviscid(x, a), (states[0],), (states[1],))
            for pt in range(2):
                g[a, pt, 0, rows, :] = scale[a] * euler[pt][0]
                for m in range(4):
                    g[a, pt, m + 1, rows, :] = scale[a] * (euler[pt][m + 1] - visc[pt][a][m])

    blocks_of(fluxes)
    for a in range(3):
        def surfaces(rows):
            primal = ([uf[0, m, a, rows, :] for m in range(5)], [of[0, m, a, rows, :] for m in range(5)])
            tangent = ([uf[1, m, a, rows, :] for m in range(5)], [of[1, m, a, rows, :] for m in range(5)])
            both = jax.jvp(
                lambda inner, outer: surface(inner, outer, sign, a), primal, tangent
            )
            scale = mf[a, rows, :]
            for pt in range(2):
                s[a, pt, 0, rows, :] = scale * both[pt][0]
                for m in range(4):
                    mine = (0.5 * LIFT) * sign * vf[a, pt, m, rows, :]
                    s[a, pt, m + 1, rows, :] = scale * (both[pt][m + 1] + mine)

        blocks_of(surfaces)

    total = derive(range(3), [g[a].reshape(10 * C, VW) for a in range(3)])
    total += lift(range(3), [s[a].reshape(10 * C, FW) for a in range(3)])
    r[...] = total.reshape(2, 5, C, VW)

    def whole_sum(parts):
        acc = parts[0]
        for part in parts[1:]:
            acc = acc + part
        return jnp.sum(jnp.sum(acc, axis=0, keepdims=True), axis=1, keepdims=True)

    pd = whole_sum([r[1, m] * u[1, m] for m in range(5)])
    dd = whole_sum([u[1, m] * u[1, m] for m in range(5)])
    mine = ratio(pd, dd)

    def put2(pt, m, a, value):
        if a == 1:
            value = jnp.where(wall, vf[a, pt, m], value)
        s[a, pt, m] = (-0.5 * LIFT) * sign * mf[a] * value

    arrived(zs2, zr2, 3)
    layer_outside(blocks2, zr2, 4, put2)

    arrived(sb2, rb2, 2)
    plane_outside(own2, rb2, 4, put2)
    lifted = lift(range(3), [s[a, :, :4].reshape(8 * C, FW) for a in range(3)])
    lifted = lifted.reshape(2, 4, C, VW)
    for pt in range(2):
        r[pt, 1:] += lifted[pt]
    rests = [r[1, m] - mine * u[1, m] for m in range(5)]
    rs = whole_sum([r[0, m] * r[0, m] for m in range(5)])
    rr = whole_sum([x * x for x in rests])
    rd = whole_sum([x * u[1, m] for m, x in enumerate(rests)])
    lane = lax.broadcasted_iota(jnp.int32, (1, 128), 1)
    row = jnp.zeros((1, 128), F32)
    for i, value in enumerate((mine, dd, rs, rr, rd)):
        row = jnp.where(lane == i, value, row)
    st[...] = row
    for k in range(1, everyone):
        pltpu.make_async_remote_copy(
            src_ref=st, dst_ref=sta.at[k], send_sem=stsem.at[0], recv_sem=stsem.at[1],
            device_id=peer(k), device_id_type=MESH,
        ).start()
    sta[0] = st[...]
    own_ref[...] = xd[1]
    for pt, part in enumerate((res_ref, prod_ref)):
        for l in range(L):
            for m in range(5):
                part[:, l, 125 * m : 125 * (m + 1)] = r[pt, m, :, 128 * l : 128 * l + 125]
    landed(sta.at[pl.ds(1, everyone - 1)], stsem.at[1])
    landed(sta.at[pl.ds(1, everyone - 1)], stsem.at[0])
    table_ref[...] = sta[...].reshape(everyone, 128)


def finish(total_count, res, prod, d, table_ref, res_hbm, basis_hbm, kry_ref, basis, sems):
    first = pltpu.make_async_copy(res, res_hbm, sems.at[0])
    first.start()
    lane = lax.broadcasted_iota(jnp.int32, (1, 128), 1)
    table = table_ref[...]
    mine, dd, rs, rr, rd = [
        jnp.sum(jnp.where(lane == i, table, 0.0), axis=1, keepdims=True) for i in range(5)
    ]
    coefficient = jnp.sum(rd + mine * dd, axis=0, keepdims=True) * (1.0 / total_count)
    shift = mine - coefficient
    rr = jnp.sum(rr + 2.0 * shift * rd + shift * shift * dd, axis=0, keepdims=True)
    rs = jnp.sum(rs, axis=0, keepdims=True)
    beta = jnp.sqrt(rr * (1.0 / total_count))
    norm = jnp.sqrt(rs * (1.0 / total_count))
    row = jnp.where(lane == 0, coefficient, jnp.where(lane == 1, beta, norm))
    kry_ref[...] = row[0, :3]
    c, inv = coefficient, 1.0 / beta
    basis[...] = (prod[...] - c[:, :, None] * d[...]) * inv[:, :, None]
    second = pltpu.make_async_copy(basis, basis_hbm, sems.at[1])
    second.start()
    first.wait()
    second.wait()


def local(ns, np_, state, direction, metric, face_source, send_rows):
    C, L, width = state.shape
    slots = send_rows.shape[2]
    SP = -(-slots // 8) * 8
    VW, FW = 128 * L, 64 * L
    own = 4 * C
    keys = np.full((2, max(3 * own, 6 * SP)), -7, np.float32)
    side, rest = np.divmod(np.arange(own), 2 * C)
    keys[0, : 3 * own] = np.tile(4 * (rest % C) + 2 * (rest // C) + side, 3)
    for copy in range(3):
        for side in range(2):
            at = (2 * copy + side) * SP
            keys[1, at : at + slots] = own + side * slots + np.arange(slots)
    tiles = 4 * (slots // 8) + -(-4 * (slots % 8) // 8)
    operands = (
        state, direction, jnp.transpose(metric, (2, 1, 0)), face_source.T, send_rows,
        jnp.asarray(keys), jnp.asarray(operators(L)),
    )
    operands = [pltpu.with_memory_space_constraint(x, pltpu.HBM) for x in operands]
    vmem = lambda *shape: pltpu.VMEM(shape, F32)
    dma = lambda n: pltpu.SemaphoreType.DMA((n,))
    spec = pl.BlockSpec(memory_space=pltpu.VMEM)
    parts, product, own, table = pl.pallas_call(
        functools.partial(kernel, ns, np_),
        out_shape=(
            *[jax.ShapeDtypeStruct(state.shape, F32)] * 3,
            jax.ShapeDtypeStruct((ns * np_, 128), F32),
        ),
        in_specs=[pl.BlockSpec(memory_space=pltpu.HBM)] * 7,
        out_specs=(spec,) * 4,
        scratch_shapes=[
            vmem(2, 5, C, VW), vmem(2, 5, 3, C, FW), vmem(2, 5, 3, C, FW),
            vmem(2, 4, C, VW), vmem(3, 2, 4, C, FW), vmem(3, 2, 4, C, VW),
            vmem(3, 2, 8, C, FW), vmem(3, 2, 4, C, FW),
            vmem(3, 2, 5, C, VW), vmem(3, 2, 5, C, FW), vmem(2, 5, C, VW),
            vmem(3, C, VW), vmem(3, C, FW),
            vmem(2, tiles, 8, FW), vmem(2, tiles, 8, FW), vmem(2, C, 3 * FW), vmem(2, C, 3 * FW),
            vmem(2, tiles, 8, FW), vmem(2, tiles, 8, FW), vmem(2, C, 2 * FW), vmem(2, C, 2 * FW),
            vmem(1, 128), vmem(ns * np_, 1, 128),
            vmem(2, C, L, width), *[pltpu.VMEM(x.shape, x.dtype) for x in operands[2:]],
            dma(4), dma(4), dma(2), dma(6),
        ],
        compiler_params=pltpu.CompilerParams(
            collective_id=0, has_side_effects=True, vmem_limit_bytes=40 * 1024 * 1024
        ),
        name="navier",
    )(*operands)
    hbm = pl.BlockSpec(memory_space=pltpu.HBM)
    return pl.pallas_call(
        functools.partial(finish, float(state.size * ns * np_)),
        out_shape=(
            jax.ShapeDtypeStruct(state.shape, F32),
            jax.ShapeDtypeStruct(state.shape, F32),
            jax.ShapeDtypeStruct((3,), F32),
        ),
        in_specs=[spec] * 4,
        out_specs=(hbm, hbm, spec),
        scratch_shapes=[vmem(C, L, width), dma(2)],
        compiler_params=pltpu.CompilerParams(vmem_limit_bytes=16 * 1024 * 1024),
        name="finish",
    )(parts, product, own, table)


def solution(mesh):
    return jax.shard_map(
        functools.partial(local, mesh.shape["stream"], mesh.shape["span"]),
        mesh=mesh,
        in_specs=(
            P("stream", "span", None),
            P("stream", "span", None),
            P("stream", "span", None),
            P("stream", None),
            P("stream", None, None),
        ),
        out_specs=(P("stream", "span", None), P("stream", "span", None), P()),
        check_vma=False,
    )
```

```python
import functools
import math

import jax
import jax.numpy as jnp
import numpy as np
from jax import lax
from jax.experimental import pallas as pl
from jax.experimental.pallas import tpu as pltpu
from jax.sharding import PartitionSpec as P

GAMMA = 1.4
VISC = 0.01
COND = VISC * GAMMA / ((GAMMA - 1.0) * 0.72)
LIFT = 10.0
MESH = pl.DeviceIdType.MESH
F32, BF16 = jnp.float32, jnp.bfloat16


def diff_table():
    spread = math.sqrt(3.0 / 7.0)
    points = np.array([-1.0, -spread, 0.0, spread, 1.0])
    weights = np.array(
        [np.prod([points[i] - points[j] for j in range(5) if j != i]) for i in range(5)]
    )
    matrix = np.zeros((5, 5))
    for i in range(5):
        for j in range(5):
            if i != j:
                matrix[i, j] = weights[i] / (weights[j] * (points[i] - points[j]))
        matrix[i, i] = np.sum([1.0 / (points[i] - points[j]) for j in range(5) if j != i])
    return matrix


def operators(layers):
    table = diff_table()
    eye = np.eye(5)
    kron = [
        np.einsum("ai,bj,ck->ijkabc", *[table if m == a else eye for m in range(3)]).reshape(125, 125)
        for a in range(3)
    ]
    node = np.arange(125).reshape(5, 5, 5)
    vw, fw, half = 128 * layers, 64 * layers, 32 * layers
    deriv = np.zeros((3, vw, vw), np.float32)
    pick = np.zeros((3, vw, fw), np.float32)
    for a in range(3):
        for l in range(layers):
            b = 128 * l
            deriv[a, b : b + 125, b : b + 125] = kron[a]
            for side in range(2):
                face = np.take(node, 4 * side, axis=a).reshape(-1)
                for m, at in enumerate(face):
                    pick[a, b + at, side * half + 32 * l + m] = 1.0
    high = deriv.astype(jnp.bfloat16)
    low = (deriv - high.astype(np.float32)).astype(jnp.bfloat16)
    lift = np.swapaxes(pick, 1, 2).astype(jnp.bfloat16)
    return np.concatenate([low, high, lift], axis=1)


def pieces(x, n):
    out = []
    for i in range(n):
        p = x.astype(BF16)
        out.append(p)
        if i + 1 < n:
            x = x - p.astype(F32)
    return out


def dot(a, b):
    return jnp.dot(a, b, preferred_element_type=F32)


def fields_of(u):
    inv = 1.0 / u[0]
    vel = [u[1] * inv, u[2] * inv, u[3] * inv]
    kinetic = 0.5 * (u[1] * vel[0] + u[2] * vel[1] + u[3] * vel[2])
    pressure = (GAMMA - 1.0) * (u[4] - kinetic)
    return vel, pressure, pressure * inv


def inviscid(u, a):
    vel, pressure, _ = fields_of(u)
    out = [u[1 + a]]
    for m in range(3):
        term = u[1 + m] * vel[a]
        out.append(term + pressure if m == a else term)
    out.append((u[4] + pressure) * vel[a])
    return out


def viscous(vel, q, a, divergence):
    stress = []
    for m in range(3):
        term = q[a][m] + q[m][a]
        if m == a:
            term = term - 2.0 / 3.0 * divergence
        stress.append(VISC * term)
    energy = stress[0] * vel[0] + stress[1] * vel[1] + stress[2] * vel[2] + COND * q[a][3]
    return stress + [energy]


def viscous_all(u, q):
    inv = 1.0 / u[0]
    vel = [u[1] * inv, u[2] * inv, u[3] * inv]
    divergence = q[0][0] + q[1][1] + q[2][2]
    return [viscous(vel, q, a, divergence) for a in range(3)]


def viscous_at(u, q, a):
    inv = 1.0 / u[0]
    vel = [u[1] * inv, u[2] * inv, u[3] * inv]
    return viscous(vel, q, a, q[0][0] + q[1][1] + q[2][2])


def gradient_fields(u):
    vel, _, temper = fields_of(u)
    return vel + [temper]


def surface(inner, outer, sign, a):
    vi, pi, ti = fields_of(inner)
    vo, po, to = fields_of(outer)
    square = sum(v * v for v in vi) + GAMMA * ti + sum(v * v for v in vo) + GAMMA * to
    speed = jnp.sqrt(0.5 * square)
    fi, fo = inviscid(inner, a), inviscid(outer, a)
    return [
        (0.5 * LIFT) * (sign * (fo[m] - fi[m]) - speed * (outer[m] - inner[m])) for m in range(5)
    ]


def ratio(top, bottom):
    return jnp.where(bottom > 0.0, top / jnp.where(bottom > 0.0, bottom, 1.0), 0.0)


def needed(a):
    return [(a, f) for f in range(4)] + [x for b in range(3) if b != a for x in ((b, a), (b, b))]


def kernel(
    ns, np_,
    x_hbm, d_hbm, metric_hbm, fs_hbm, sr_hbm, key_hbm, ops_hbm,
    res_ref, prod_ref, own_ref, table_ref,
    u, uf, of, w, jf, q, qf, vf, g, s, r, mv, mf,
    sb1, rb1, zs1, zr1, sb2, rb2, zs2, zr2, st, sta,
    xd, metric_ref, fs_ref, sr_ref, key_ref, ops_ref,
    xsend, xrecv, stsem, loads, word,
):
    C, L = xd.shape[1], xd.shape[2]
    VW, FW, half = 128 * L, 64 * L, 32 * L
    SLOTS = sr_ref.shape[2]
    SP = -(-SLOTS // 8) * 8
    MAIN, REM = SLOTS // 8, SLOTS % 8
    OWN = 4 * C
    ms, mp = lax.axis_index("stream"), lax.axis_index("span")
    lower, upper = lax.rem(ms + ns - 1, ns), lax.rem(ms + 1, ns)
    below, above = lax.rem(mp + np_ - 1, np_), lax.rem(mp + 1, np_)

    inputs = [
        pltpu.make_async_copy(src, dst, loads.at[i])
        for src, dst, i in [
            (x_hbm, xd.at[0], 0), (d_hbm, xd.at[1], 0), (key_hbm, key_ref, 1), (fs_hbm, fs_ref, 2),
            (sr_hbm, sr_ref, 3), (metric_hbm, metric_ref, 4), (ops_hbm, ops_ref, 5),
        ]
    ]
    for copy in inputs:
        copy.start()

    def peer(k):
        a, b = divmod(k, np_)
        return lax.rem(ms + a, ns), lax.rem(mp + b, np_)

    everyone = ns * np_
    rounds = 4 if ns == 8 else 0
    near = [np_, everyone - np_, *range(1, np_)]
    greeted = near if rounds else list(range(1, everyone))
    barrier = pltpu.get_barrier_semaphore()
    for k in greeted:
        pl.semaphore_signal(barrier, inc=1, device_id=peer(k), device_id_type=MESH)

    def pass_on(i):
        for side, to in ((0, lower), (1, upper)):
            if i > 0:
                pl.semaphore_wait(word.at[i - 1, side], 1)
        if i < rounds:
            for side, to in ((0, lower), (1, upper)):
                pl.semaphore_signal(
                    word.at[i, 1 - side], inc=1, device_id=(to, mp), device_id_type=MESH
                )

    fl = lax.broadcasted_iota(jnp.int32, (1, FW), 1)
    vl = lax.broadcasted_iota(jnp.int32, (1, VW), 1)
    first = fl < half
    sign = jnp.where(first, -1.0, 1.0)
    flayer = lax.rem(fl, half) // 32
    fnode = lax.rem(fl, 32)
    fside = jnp.where(first, 0, 1)
    major, minor = fnode // 5, lax.rem(fnode, 5)
    nodes = [
        jnp.where(fnode < 25, at, 127)
        for at in (100 * fside + fnode, 25 * major + 20 * fside + minor, 5 * fnode + 4 * fside)
    ]

    def pull(x, at):
        return jnp.take_along_axis(
            x, jnp.broadcast_to(at, x.shape), axis=1, mode="promise_in_bounds"
        )

    def trace(volume, a):
        value = None
        for l in range(L):
            part = pull(volume[:, 128 * l : 128 * (l + 1)], nodes[a])
            value = part if value is None else jnp.where(flayer == l, part, value)
        return value

    def edge(a, b):
        at = dict(zip([x for x in range(3) if x != a], (major, minor)))
        at[a] = 4 * fside
        one, two = [x for x in range(3) if x != b]
        there = (lax.rem(at[b], 4) == 0) & (fnode < 25)
        lane = half * (at[b] // 4) + 32 * flayer + 5 * at[one] + at[two]
        return there, jnp.where(there, lane, 0)

    edges = {(a, b): edge(a, b) for a in range(3) for b in range(3) if a != b}

    def roll(x, shift):
        shift = shift % FW
        return pltpu.roll(x, shift, 1) if shift else x

    di = lax.broadcasted_iota(jnp.int32, (C, C), 0)
    dj = lax.broadcasted_iota(jnp.int32, (C, C), 1)

    def column(row):
        return jnp.sum(jnp.where(di == dj, row, 0.0), axis=1, keepdims=True)

    def blocks_of(body):
        @pl.loop(0, C // 8, unroll=True)
        def _(i):
            body(pl.ds(pl.multiple_of(i * 8, 8), 8))

    def lift(axes, values):
        halves, table = [], []
        for a, value in zip(axes, values):
            halves += pieces(value, 2)
            table += [ops_ref[a, 2 * VW :]] * 2
        return dot(jnp.concatenate(halves, axis=1), jnp.concatenate(table, axis=0))

    def derive(axes, values):
        halves, table = [], []
        for a, value in zip(axes, values):
            high, low = pieces(value, 2)
            halves += [high, low, high]
            table += [ops_ref[a, : 2 * VW], ops_ref[a, VW : 2 * VW]]
        return dot(jnp.concatenate(halves, axis=1), jnp.concatenate(table, axis=0))

    def choose(hot, x, depth=3):
        return dot(hot[:, : depth * x.shape[0]], jnp.concatenate(pieces(x, depth)[::-1], axis=0))

    def swap(a, b):
        return (
            jnp.where(first, a, pltpu.roll(b, half, 1)),
            jnp.where(first, pltpu.roll(a, half, 1), b),
        )

    def landed(ref, sem):
        pltpu.make_async_copy(ref, ref, sem).wait()

    def remote(pairs, base):
        for src, dst, to in pairs:
            pltpu.make_async_remote_copy(
                src_ref=src, dst_ref=dst, send_sem=xsend.at[base],
                recv_sem=xrecv.at[base], device_id=to, device_id_type=MESH,
            ).start()

    def arrived(source, target, base):
        landed(target, xrecv.at[base])
        landed(source, xsend.at[base])

    def plane_pack(faces, members, sb):
        blocks = [[swap(faces(0, m, a), faces(1, m, a)) for m in range(members)] for a in range(2)]
        table = jnp.concatenate(
            [
                jnp.concatenate([blocks[a][m][side] for m in range(members)], axis=1)
                for side in range(2)
                for a in range(2)
            ],
            axis=0,
        )
        sent = choose(send_hot, table)
        for m in range(4):
            value = sent[:, FW * m : FW * (m + 1)]
            if members > 4:
                spare = roll(sent[:, 4 * FW :], 25 - 7 * m)
                value = jnp.where(fnode < 25, value, spare)
            for side in range(2):
                for b in range(MAIN):
                    at = side * SP + 8 * b
                    sb[side, 4 * b + m] = value[at : at + 8]
                for e in range(REM):
                    at, to = side * SP + 8 * MAIN + e, REM * m + e
                    sb[side, 4 * MAIN + to // 8, to % 8 : to % 8 + 1, :] = value[at : at + 1]
        return table

    def plane_send(sb, rb, base):
        remote([(sb.at[0], rb.at[1], (lower, mp)), (sb.at[1], rb.at[0], (upper, mp))], base)

    def layer_send(faces, members, zs, zr, base):
        blocks = [swap(faces(0, m, 2), faces(1, m, 2)) for m in range(members)]
        for m in range(0, members, 2):
            for side in range(2):
                value = blocks[m][side]
                if m + 1 < members:
                    other = roll(blocks[m + 1][side], 32 if side == 0 else -32)
                    value = jnp.where(flayer == (0 if side == 0 else L - 1), value, other)
                zs[side, :, FW * (m // 2) : FW * (m // 2 + 1)] = value
        remote([(zs.at[0], zr.at[1], (ms, below)), (zs.at[1], zr.at[0], (ms, above))], base)
        return blocks

    def plane_outside(own, rb, members, put, depth):
        lanes = lax.broadcasted_iota(jnp.int32, (1, members * FW), 1)
        member, node = lanes // FW, lax.rem(lanes, 32)
        row8 = lax.broadcasted_iota(jnp.int32, (8, 1), 0)
        rows = []
        for side in range(2):
            rows += [
                jnp.concatenate([rb[side, 4 * b + m] for m in range(4)], axis=1)
                for b in range(MAIN)
            ]
            if REM:
                parts = []
                for m in range(4):
                    part = jnp.zeros((8, FW), F32)
                    for e in range(REM):
                        to = REM * m + e
                        line = rb[side, 4 * MAIN + to // 8, to % 8 : to % 8 + 1, :]
                        part = jnp.where(row8 == e, line, part)
                    parts.append(part)
                rows.append(jnp.concatenate(parts, axis=1))
        received = jnp.concatenate(rows, axis=0)
        if members * FW > received.shape[1]:
            spare = jnp.zeros((2 * SP, FW), F32)
            for m in range(received.shape[1] // FW):
                part = roll(received[:, FW * m : FW * (m + 1)], 7 * m - 25)
                spare = jnp.where((fnode >= 7 * m) & (fnode < 7 * m + 7), part, spare)
            received = jnp.concatenate([received, spare], axis=1)
            pad = jnp.where(lax.rem(member, 4) == 0, 1.0, 0.0)
            received = jnp.where(node < 25, received, pad)
        got = own + choose(hot_recv, received, depth)
        for a in range(2):
            for m in range(members):
                lanes = slice(FW * m, FW * (m + 1))
                lo = got[a * C : (a + 1) * C, lanes]
                hi = got[(2 + a) * C : (3 + a) * C, lanes]
                primal, tangent = swap(lo, hi)
                put(0, m, a, primal)
                put(1, m, a, tangent)

    def layer_outside(blocks, zr, members, put):
        for m in range(members):
            lanes = slice(FW * (m // 2), FW * (m // 2 + 1))
            step = 32 * (L - 1 if m % 2 == 0 else L - 2)
            lo = jnp.where(flayer == 0, roll(zr[0, :, lanes], -step), roll(blocks[m][1], 32))
            hi = jnp.where(flayer == L - 1, roll(zr[1, :, lanes], step), roll(blocks[m][0], -32))
            primal, tangent = swap(lo, hi)
            put(0, m, 2, primal)
            put(1, m, 2, tangent)

    landed(xd, loads.at[0])
    for pt in range(2):
        for l in range(L):
            for m in range(5):
                pad = 1.0 if pt == 0 and m % 4 == 0 else 0.0
                u[pt, m, :, 128 * l + 120 : 128 * (l + 1)] = jnp.full((C, 8), pad, F32)
                u[pt, m, :, 128 * l : 128 * l + 125] = xd[pt, :, l, 125 * m : 125 * (m + 1)]
    for copy in inputs[2:6]:
        copy.wait()
    own_keys, recv_keys = key_ref[0:1, : 3 * OWN], key_ref[1:2, : 6 * SP]
    ri = lax.broadcasted_iota(jnp.int32, (SP, SLOTS), 0)
    li = lax.broadcasted_iota(jnp.int32, (SP, SLOTS), 1)
    send_hot = []
    for side in range(2):
        row = sr_ref[0, side : side + 1, :].astype(F32)
        wanted = jnp.sum(jnp.where(ri == li, row, 0.0), axis=1, keepdims=True)
        send_hot.append(jnp.where(wanted == own_keys, 1.0, 0.0))
    send_hot = jnp.concatenate(send_hot, axis=0).astype(BF16)

    def state_faces(a):
        for pt in range(2):
            for m in range(5):
                uf[pt, m, a] = trace(u[pt, m], a)

    state_faces(0)
    state_faces(1)
    table1 = plane_pack(lambda pt, m, a: uf[pt, m, a], 5, sb1)
    pl.semaphore_wait(barrier, len(greeted))
    plane_send(sb1, rb1, 0)
    if rounds:
        pass_on(0)
    state_faces(2)
    blocks1 = layer_send(lambda pt, m, a: uf[pt, m, a], 5, zs1, zr1, 1)

    source = [column(fs_ref[f : f + 1, :].astype(F32)) for f in range(4)]

    def hot(keys):
        rows = [jnp.where(source[2 * a + side] == keys, 1.0, 0.0) for side in range(2) for a in range(2)]
        return jnp.concatenate(rows, axis=0).astype(BF16)

    hot_own, hot_recv = hot(own_keys), hot(recv_keys)
    for a in range(3):
        wide = jnp.zeros((C, VW), F32)
        face = jnp.zeros((C, FW), F32)
        for l in range(L):
            value = column(metric_ref[a, l : l + 1, :])
            wide = jnp.where(vl // 128 == l, value, wide)
            face = jnp.where(flayer == l, value, face)
        mv[a] = wide
        mf[a] = face

    def gradients(rows):
        primal = [u[0, m, rows, :] for m in range(5)]
        tangent = [u[1, m, rows, :] for m in range(5)]
        fp, ft = jax.jvp(gradient_fields, (primal,), (tangent,))
        for m in range(4):
            w[0, m, rows, :] = fp[m]
            w[1, m, rows, :] = ft[m]

    blocks_of(gradients)
    inputs[6].wait()
    own1 = choose(hot_own, table1)
    fields = w[...].reshape(8 * C, VW)
    for a in range(3):
        q[a] = derive([a], [fields]).reshape(2, 4, C, VW)
    for a in range(3):
        for pt in range(2):
            for n, (b, f) in enumerate(needed(a)):
                qf[a, pt, n] = trace(q[b, pt, f], a)

    low_wall = jnp.where(source[2] < 0.0, 1.0, 0.0)
    high_wall = jnp.where(source[3] < 0.0, 1.0, 0.0)
    wall = jnp.where(first, low_wall, high_wall) > 0.5

    def put1(pt, m, a, value):
        if a == 1:
            own = uf[pt, m, a]
            value = jnp.where(wall, own if m % 4 == 0 else -own, value)
        of[pt, m, a] = value

    def face_fields(table, a, rows):
        primal = [table[0, m, a, rows, :] for m in range(5)]
        tangent = [table[1, m, a, rows, :] for m in range(5)]
        return jax.jvp(gradient_fields, (primal,), (tangent,))

    def insides(a):
        def body(rows):
            both = face_fields(uf, a, rows)
            for pt in range(2):
                for m in range(4):
                    jf[a, pt, m, rows, :] = both[pt][m]

        blocks_of(body)

    def jumps(a):
        def body(rows):
            both = face_fields(of, a, rows)
            for pt in range(2):
                for m in range(4):
                    jump = both[pt][m] - jf[a, pt, m, rows, :]
                    jf[a, pt, m, rows, :] = (0.5 * LIFT) * sign * jump

        blocks_of(body)

    for a in range(3):
        insides(a)

    def edge_jumps(a, b):
        there, lane = edges[a, b]
        for n, (other, f) in enumerate(needed(a)):
            if other == b:
                for pt in range(2):
                    qf[a, pt, n] += jnp.where(there, pull(jf[b, pt, f], lane), 0.0)

    arrived(zs1, zr1, 1)
    if rounds:
        pass_on(1)
    layer_outside(blocks1, zr1, 5, put1)
    jumps(2)
    edge_jumps(0, 2)
    edge_jumps(1, 2)
    arrived(sb1, rb1, 0)
    if rounds:
        pass_on(2)
    plane_outside(own1, rb1, 5, put1, 3)
    jumps(0)
    jumps(1)
    edge_jumps(0, 1)
    edge_jumps(1, 0)

    def face_viscous(a):
        def body(rows):
            states = [[uf[pt, m, a, rows, :] for m in range(5)] for pt in range(2)]
            grads = []
            for pt in range(2):
                grad = [[None] * 4 for _ in range(3)]
                for n, (b, f) in enumerate(needed(a)):
                    value = qf[a, pt, n, rows, :]
                    if b == a:
                        value = value + jf[a, pt, f, rows, :]
                    grad[b][f] = mf[b, rows, :] * value
                grads.append(grad)
            vp, vt = jax.jvp(
                lambda x, y: viscous_at(x, y, a), (states[0], grads[0]), (states[1], grads[1])
            )
            for m in range(4):
                vf[a, 0, m, rows, :] = vp[m]
                vf[a, 1, m, rows, :] = vt[m]

        blocks_of(body)

    face_viscous(0)
    face_viscous(1)
    table2 = plane_pack(lambda pt, m, a: vf[a, pt, m], 4, sb2)
    plane_send(sb2, rb2, 2)
    edge_jumps(2, 0)
    edge_jumps(2, 1)
    face_viscous(2)
    blocks2 = layer_send(lambda pt, m, a: vf[a, pt, m], 4, zs2, zr2, 3)

    own2 = choose(hot_own, table2)
    for a in range(3):
        q[a] += lift([a], [jf[a].reshape(8 * C, FW)]).reshape(2, 4, C, VW)

    def fluxes(rows):
        scale = [mv[a, rows, :] for a in range(3)]
        states = [[u[pt, m, rows, :] for m in range(5)] for pt in range(2)]
        grads = [
            [[scale[a] * q[a, pt, m, rows, :] for m in range(4)] for a in range(3)]
            for pt in range(2)
        ]
        visc = jax.jvp(viscous_all, (states[0], grads[0]), (states[1], grads[1]))
        for a in range(3):
            euler = jax.jvp(lambda x: inviscid(x, a), (states[0],), (states[1],))
            for pt in range(2):
                g[a, pt, 0, rows, :] = scale[a] * euler[pt][0]
                for m in range(4):
                    g[a, pt, m + 1, rows, :] = scale[a] * (euler[pt][m + 1] - visc[pt][a][m])

    blocks_of(fluxes)
    if rounds:
        pass_on(3)
    for a in range(3):
        def surfaces(rows):
            primal = ([uf[0, m, a, rows, :] for m in range(5)], [of[0, m, a, rows, :] for m in range(5)])
            tangent = ([uf[1, m, a, rows, :] for m in range(5)], [of[1, m, a, rows, :] for m in range(5)])
            both = jax.jvp(
                lambda inner, outer: surface(inner, outer, sign, a), primal, tangent
            )
            scale = mf[a, rows, :]
            for pt in range(2):
                s[a, pt, 0, rows, :] = scale * both[pt][0]
                for m in range(4):
                    mine = (0.5 * LIFT) * sign * vf[a, pt, m, rows, :]
                    s[a, pt, m + 1, rows, :] = scale * (both[pt][m + 1] + mine)

        blocks_of(surfaces)

    total = derive(range(3), [g[a].reshape(10 * C, VW) for a in range(3)])
    total += lift(range(3), [s[a].reshape(10 * C, FW) for a in range(3)])
    r[...] = total.reshape(2, 5, C, VW)

    def whole_sum(parts):
        acc = parts[0]
        for part in parts[1:]:
            acc = acc + part
        return jnp.sum(jnp.sum(acc, axis=0, keepdims=True), axis=1, keepdims=True)

    pd = whole_sum([r[1, m] * u[1, m] for m in range(5)])
    dd = whole_sum([u[1, m] * u[1, m] for m in range(5)])
    mine = ratio(pd, dd)

    def put2(pt, m, a, value):
        if a == 1:
            value = jnp.where(wall, vf[a, pt, m], value)
        s[a, pt, m] = (-0.5 * LIFT) * sign * mf[a] * value

    arrived(zs2, zr2, 3)
    layer_outside(blocks2, zr2, 4, put2)

    arrived(sb2, rb2, 2)
    if rounds:
        pass_on(4)
    plane_outside(own2, rb2, 4, put2, 2)
    lifted = lift(range(3), [s[a, :, :4].reshape(8 * C, FW) for a in range(3)])
    lifted = lifted.reshape(2, 4, C, VW)
    for pt in range(2):
        r[pt, 1:] += lifted[pt]
    rests = [r[1, m] - mine * u[1, m] for m in range(5)]
    rs = whole_sum([r[0, m] * r[0, m] for m in range(5)])
    rr = whole_sum([x * x for x in rests])
    rd = whole_sum([x * u[1, m] for m, x in enumerate(rests)])
    lane = lax.broadcasted_iota(jnp.int32, (1, 128), 1)
    row = jnp.zeros((1, 128), F32)
    for i, value in enumerate((mine, dd, rs, rr, rd)):
        row = jnp.where(lane == i, value, row)
    st[...] = row
    for k in range(1, everyone):
        pltpu.make_async_remote_copy(
            src_ref=st, dst_ref=sta.at[k], send_sem=stsem.at[0], recv_sem=stsem.at[1],
            device_id=peer(k), device_id_type=MESH,
        ).start()
    sta[0] = st[...]
    own_ref[...] = xd[1]
    for pt, part in enumerate((res_ref, prod_ref)):
        for l in range(L):
            for m in range(5):
                part[:, l, 125 * m : 125 * (m + 1)] = r[pt, m, :, 128 * l : 128 * l + 125]
    landed(sta.at[pl.ds(1, everyone - 1)], stsem.at[1])
    landed(sta.at[pl.ds(1, everyone - 1)], stsem.at[0])
    table_ref[...] = sta[...].reshape(everyone, 128)


def finish(total_count, res, prod, d, table_ref, res_hbm, basis_hbm, kry_hbm, basis, kry, sems):
    first = pltpu.make_async_copy(res, res_hbm, sems.at[0])
    first.start()
    lane = lax.broadcasted_iota(jnp.int32, (1, 128), 1)
    table = table_ref[...]
    mine, dd, rs, rr, rd = [
        jnp.sum(jnp.where(lane == i, table, 0.0), axis=1, keepdims=True) for i in range(5)
    ]
    coefficient = jnp.sum(rd + mine * dd, axis=0, keepdims=True) * (1.0 / total_count)
    shift = mine - coefficient
    rr = jnp.sum(rr + 2.0 * shift * rd + shift * shift * dd, axis=0, keepdims=True)
    rs = jnp.sum(rs, axis=0, keepdims=True)
    beta = jnp.sqrt(rr * (1.0 / total_count))
    norm = jnp.sqrt(rs * (1.0 / total_count))
    row = jnp.where(lane == 0, coefficient, jnp.where(lane == 1, beta, norm))
    kry[...] = row[0, :3]
    third = pltpu.make_async_copy(kry, kry_hbm, sems.at[2])
    third.start()
    c, inv = coefficient, 1.0 / beta
    basis[...] = (prod[...] - c[:, :, None] * d[...]) * inv[:, :, None]
    second = pltpu.make_async_copy(basis, basis_hbm, sems.at[1])
    second.start()
    first.wait()
    third.wait()
    second.wait()


def local(ns, np_, state, direction, metric, face_source, send_rows):
    C, L, width = state.shape
    slots = send_rows.shape[2]
    SP = -(-slots // 8) * 8
    VW, FW = 128 * L, 64 * L
    own = 4 * C
    keys = np.full((2, max(3 * own, 6 * SP)), -7, np.float32)
    side, rest = np.divmod(np.arange(own), 2 * C)
    keys[0, : 3 * own] = np.tile(4 * (rest % C) + 2 * (rest // C) + side, 3)
    for copy in range(3):
        for side in range(2):
            at = (2 * copy + side) * SP
            keys[1, at : at + slots] = own + side * slots + np.arange(slots)
    tiles = 4 * (slots // 8) + -(-4 * (slots % 8) // 8)
    operands = (
        state, direction, jnp.transpose(metric, (2, 1, 0)), face_source.T, send_rows,
        jnp.asarray(keys), jnp.asarray(operators(L)),
    )
    operands = [pltpu.with_memory_space_constraint(x, pltpu.HBM) for x in operands]
    vmem = lambda *shape: pltpu.VMEM(shape, F32)
    dma = lambda n: pltpu.SemaphoreType.DMA((n,))
    spec = pl.BlockSpec(memory_space=pltpu.VMEM)
    parts, product, own, table = pl.pallas_call(
        functools.partial(kernel, ns, np_),
        out_shape=(
            *[jax.ShapeDtypeStruct(state.shape, F32)] * 3,
            jax.ShapeDtypeStruct((ns * np_, 128), F32),
        ),
        in_specs=[pl.BlockSpec(memory_space=pltpu.HBM)] * 7,
        out_specs=(spec,) * 4,
        scratch_shapes=[
            vmem(2, 5, C, VW), vmem(2, 5, 3, C, FW), vmem(2, 5, 3, C, FW),
            vmem(2, 4, C, VW), vmem(3, 2, 4, C, FW), vmem(3, 2, 4, C, VW),
            vmem(3, 2, 8, C, FW), vmem(3, 2, 4, C, FW),
            vmem(3, 2, 5, C, VW), vmem(3, 2, 5, C, FW), vmem(2, 5, C, VW),
            vmem(3, C, VW), vmem(3, C, FW),
            vmem(2, tiles, 8, FW), vmem(2, tiles, 8, FW), vmem(2, C, 3 * FW), vmem(2, C, 3 * FW),
            vmem(2, tiles, 8, FW), vmem(2, tiles, 8, FW), vmem(2, C, 2 * FW), vmem(2, C, 2 * FW),
            vmem(1, 128), vmem(ns * np_, 1, 128),
            vmem(2, C, L, width), *[pltpu.VMEM(x.shape, x.dtype) for x in operands[2:]],
            dma(4), dma(4), dma(2), dma(6), pltpu.SemaphoreType.REGULAR((4, 2)),
        ],
        compiler_params=pltpu.CompilerParams(
            collective_id=0, has_side_effects=True, vmem_limit_bytes=40 * 1024 * 1024
        ),
        name="navier",
    )(*operands)
    hbm = pl.BlockSpec(memory_space=pltpu.HBM)
    return pl.pallas_call(
        functools.partial(finish, float(state.size * ns * np_)),
        out_shape=(
            jax.ShapeDtypeStruct(state.shape, F32),
            jax.ShapeDtypeStruct(state.shape, F32),
            jax.ShapeDtypeStruct((3,), F32),
        ),
        in_specs=[spec] * 4,
        out_specs=(hbm, hbm, hbm),
        scratch_shapes=[vmem(C, L, width), vmem(3), dma(3)],
        compiler_params=pltpu.CompilerParams(vmem_limit_bytes=16 * 1024 * 1024),
        name="finish",
    )(parts, product, own, table)


def solution(mesh):
    return jax.shard_map(
        functools.partial(local, mesh.shape["stream"], mesh.shape["span"]),
        mesh=mesh,
        in_specs=(
            P("stream", "span", None),
            P("stream", "span", None),
            P("stream", "span", None),
            P("stream", None),
            P("stream", None, None),
        ),
        out_specs=(P("stream", "span", None), P("stream", "span", None), P()),
        check_vma=False,
    )
```

```python
import functools
import math

import jax
import jax.numpy as jnp
import numpy as np
from jax import lax
from jax.experimental import pallas as pl
from jax.experimental.pallas import tpu as pltpu
from jax.sharding import PartitionSpec as P

GAMMA = 1.4
VISC = 0.01
COND = VISC * GAMMA / ((GAMMA - 1.0) * 0.72)
LIFT = 10.0
MESH = pl.DeviceIdType.MESH
F32, BF16 = jnp.float32, jnp.bfloat16


def diff_table():
    spread = math.sqrt(3.0 / 7.0)
    points = np.array([-1.0, -spread, 0.0, spread, 1.0])
    weights = np.array(
        [np.prod([points[i] - points[j] for j in range(5) if j != i]) for i in range(5)]
    )
    matrix = np.zeros((5, 5))
    for i in range(5):
        for j in range(5):
            if i != j:
                matrix[i, j] = weights[i] / (weights[j] * (points[i] - points[j]))
        matrix[i, i] = np.sum([1.0 / (points[i] - points[j]) for j in range(5) if j != i])
    return matrix


def operators(layers):
    table = diff_table()
    eye = np.eye(5)
    kron = [
        np.einsum("ai,bj,ck->ijkabc", *[table if m == a else eye for m in range(3)]).reshape(125, 125)
        for a in range(3)
    ]
    node = np.arange(125).reshape(5, 5, 5)
    vw, fw, half = 128 * layers, 64 * layers, 32 * layers
    deriv = np.zeros((3, vw, vw), np.float32)
    pick = np.zeros((3, vw, fw), np.float32)
    for a in range(3):
        for l in range(layers):
            b = 128 * l
            deriv[a, b : b + 125, b : b + 125] = kron[a]
            for side in range(2):
                face = np.take(node, 4 * side, axis=a).reshape(-1)
                for m, at in enumerate(face):
                    pick[a, b + at, side * half + 32 * l + m] = 1.0
    high = deriv.astype(jnp.bfloat16)
    low = (deriv - high.astype(np.float32)).astype(jnp.bfloat16)
    lift = np.swapaxes(pick, 1, 2).astype(jnp.bfloat16)
    return np.concatenate([low, high, lift], axis=1)


def pieces(x, n):
    out = []
    for i in range(n):
        p = x.astype(BF16)
        out.append(p)
        if i + 1 < n:
            x = x - p.astype(F32)
    return out


def dot(a, b):
    return jnp.dot(a, b, preferred_element_type=F32)


def fields_of(u):
    inv = 1.0 / u[0]
    vel = [u[1] * inv, u[2] * inv, u[3] * inv]
    kinetic = 0.5 * (u[1] * vel[0] + u[2] * vel[1] + u[3] * vel[2])
    pressure = (GAMMA - 1.0) * (u[4] - kinetic)
    return vel, pressure, pressure * inv


def inviscid(u, a):
    vel, pressure, _ = fields_of(u)
    out = [u[1 + a]]
    for m in range(3):
        term = u[1 + m] * vel[a]
        out.append(term + pressure if m == a else term)
    out.append((u[4] + pressure) * vel[a])
    return out


def viscous(vel, q, a, divergence):
    stress = []
    for m in range(3):
        term = q[a][m] + q[m][a]
        if m == a:
            term = term - 2.0 / 3.0 * divergence
        stress.append(VISC * term)
    energy = stress[0] * vel[0] + stress[1] * vel[1] + stress[2] * vel[2] + COND * q[a][3]
    return stress + [energy]


def viscous_all(u, q):
    inv = 1.0 / u[0]
    vel = [u[1] * inv, u[2] * inv, u[3] * inv]
    divergence = q[0][0] + q[1][1] + q[2][2]
    return [viscous(vel, q, a, divergence) for a in range(3)]


def viscous_at(u, q, a):
    inv = 1.0 / u[0]
    vel = [u[1] * inv, u[2] * inv, u[3] * inv]
    return viscous(vel, q, a, q[0][0] + q[1][1] + q[2][2])


def gradient_fields(u):
    vel, _, temper = fields_of(u)
    return vel + [temper]


def surface(inner, outer, sign, a):
    vi, pi, ti = fields_of(inner)
    vo, po, to = fields_of(outer)
    square = sum(v * v for v in vi) + GAMMA * ti + sum(v * v for v in vo) + GAMMA * to
    speed = jnp.sqrt(0.5 * square)
    fi, fo = inviscid(inner, a), inviscid(outer, a)
    return [
        (0.5 * LIFT) * (sign * (fo[m] - fi[m]) - speed * (outer[m] - inner[m])) for m in range(5)
    ]


def ratio(top, bottom):
    return jnp.where(bottom > 0.0, top / jnp.where(bottom > 0.0, bottom, 1.0), 0.0)


def needed(a):
    return [(a, f) for f in range(4)] + [x for b in range(3) if b != a for x in ((b, a), (b, b))]


def kernel(
    ns, np_,
    x_hbm, d_hbm, metric_hbm, fs_hbm, sr_hbm, key_hbm, ops_hbm,
    res_ref, prod_ref, own_ref, table_ref,
    u, uf, of, w, jf, q, qf, vf, g, s, r, mv, mf,
    sb1, rb1, zs1, zr1, sb2, rb2, zs2, zr2, st, sta,
    xd, metric_ref, fs_ref, sr_ref, key_ref, ops_ref,
    xsend, xrecv, stsem, loads, word,
):
    C, L = xd.shape[1], xd.shape[2]
    VW, FW, half = 128 * L, 64 * L, 32 * L
    SLOTS = sr_ref.shape[2]
    SP = -(-SLOTS // 8) * 8
    MAIN, REM = SLOTS // 8, SLOTS % 8
    OWN = 4 * C
    ms, mp = lax.axis_index("stream"), lax.axis_index("span")
    lower, upper = lax.rem(ms + ns - 1, ns), lax.rem(ms + 1, ns)
    below, above = lax.rem(mp + np_ - 1, np_), lax.rem(mp + 1, np_)

    inputs = [
        pltpu.make_async_copy(src, dst, loads.at[i])
        for src, dst, i in [
            (x_hbm, xd.at[0], 0), (d_hbm, xd.at[1], 0), (key_hbm, key_ref, 1), (fs_hbm, fs_ref, 2),
            (sr_hbm, sr_ref, 3), (metric_hbm, metric_ref, 4), (ops_hbm, ops_ref, 5),
        ]
    ]
    for copy in inputs:
        copy.start()

    def peer(k):
        a, b = divmod(k, np_)
        return lax.rem(ms + a, ns), lax.rem(mp + b, np_)

    everyone = ns * np_
    relayed = ns == 8
    near = [a * np_ for a in (1, 2, ns - 2, ns - 1)]
    greeted = near + list(range(1, np_)) if relayed else list(range(1, everyone))
    barrier = pltpu.get_barrier_semaphore()
    for k in greeted:
        pl.semaphore_signal(barrier, inc=1, device_id=peer(k), device_id_type=MESH)

    def vouch(which, base):
        for i, k in enumerate(which):
            pl.semaphore_signal(word.at[base + i], inc=1, device_id=peer(k), device_id_type=MESH)

    def vouched(which, base):
        for i in range(len(which)):
            pl.semaphore_wait(word.at[base + i], 1)

    fl = lax.broadcasted_iota(jnp.int32, (1, FW), 1)
    vl = lax.broadcasted_iota(jnp.int32, (1, VW), 1)
    first = fl < half
    sign = jnp.where(first, -1.0, 1.0)
    flayer = lax.rem(fl, half) // 32
    fnode = lax.rem(fl, 32)
    fside = jnp.where(first, 0, 1)
    major, minor = fnode // 5, lax.rem(fnode, 5)
    nodes = [
        jnp.where(fnode < 25, at, 127)
        for at in (100 * fside + fnode, 25 * major + 20 * fside + minor, 5 * fnode + 4 * fside)
    ]

    def pull(x, at):
        return jnp.take_along_axis(
            x, jnp.broadcast_to(at, x.shape), axis=1, mode="promise_in_bounds"
        )

    def trace(volume, a):
        value = None
        for l in range(L):
            part = pull(volume[:, 128 * l : 128 * (l + 1)], nodes[a])
            value = part if value is None else jnp.where(flayer == l, part, value)
        return value

    def edge(a, b):
        at = dict(zip([x for x in range(3) if x != a], (major, minor)))
        at[a] = 4 * fside
        one, two = [x for x in range(3) if x != b]
        there = (lax.rem(at[b], 4) == 0) & (fnode < 25)
        lane = half * (at[b] // 4) + 32 * flayer + 5 * at[one] + at[two]
        return there, jnp.where(there, lane, 0)

    edges = {(a, b): edge(a, b) for a in range(3) for b in range(3) if a != b}

    def roll(x, shift):
        shift = shift % FW
        return pltpu.roll(x, shift, 1) if shift else x

    di = lax.broadcasted_iota(jnp.int32, (C, C), 0)
    dj = lax.broadcasted_iota(jnp.int32, (C, C), 1)

    def column(row):
        return jnp.sum(jnp.where(di == dj, row, 0.0), axis=1, keepdims=True)

    def blocks_of(body):
        @pl.loop(0, C // 8, unroll=True)
        def _(i):
            body(pl.ds(pl.multiple_of(i * 8, 8), 8))

    def lift(axes, values):
        halves, table = [], []
        for a, value in zip(axes, values):
            halves += pieces(value, 2)
            table += [ops_ref[a, 2 * VW :]] * 2
        return dot(jnp.concatenate(halves, axis=1), jnp.concatenate(table, axis=0))

    def derive(axes, values):
        halves, table = [], []
        for a, value in zip(axes, values):
            high, low = pieces(value, 2)
            halves += [high, low, high]
            table += [ops_ref[a, : 2 * VW], ops_ref[a, VW : 2 * VW]]
        return dot(jnp.concatenate(halves, axis=1), jnp.concatenate(table, axis=0))

    def choose(hot, x, depth=3):
        return dot(hot[:, : depth * x.shape[0]], jnp.concatenate(pieces(x, depth)[::-1], axis=0))

    def swap(a, b):
        return (
            jnp.where(first, a, pltpu.roll(b, half, 1)),
            jnp.where(first, pltpu.roll(a, half, 1), b),
        )

    def landed(ref, sem):
        pltpu.make_async_copy(ref, ref, sem).wait()

    def remote(pairs, base):
        for src, dst, to in pairs:
            pltpu.make_async_remote_copy(
                src_ref=src, dst_ref=dst, send_sem=xsend.at[base],
                recv_sem=xrecv.at[base], device_id=to, device_id_type=MESH,
            ).start()

    def arrived(source, target, base):
        landed(target, xrecv.at[base])
        landed(source, xsend.at[base])

    def plane_pack(faces, members, sb):
        blocks = [[swap(faces(0, m, a), faces(1, m, a)) for m in range(members)] for a in range(2)]
        table = jnp.concatenate(
            [
                jnp.concatenate([blocks[a][m][side] for m in range(members)], axis=1)
                for side in range(2)
                for a in range(2)
            ],
            axis=0,
        )
        sent = choose(send_hot, table)
        for m in range(4):
            value = sent[:, FW * m : FW * (m + 1)]
            if members > 4:
                spare = roll(sent[:, 4 * FW :], 25 - 7 * m)
                value = jnp.where(fnode < 25, value, spare)
            for side in range(2):
                for b in range(MAIN):
                    at = side * SP + 8 * b
                    sb[side, 4 * b + m] = value[at : at + 8]
                for e in range(REM):
                    at, to = side * SP + 8 * MAIN + e, REM * m + e
                    sb[side, 4 * MAIN + to // 8, to % 8 : to % 8 + 1, :] = value[at : at + 1]
        return table

    def plane_send(sb, rb, base):
        far = lax.rem(ms, 2)
        to = [lax.rem(ms + ns - 1 + 2 * side, ns) for side in (far, 1 - far)]
        remote(
            [(sb.at[side], rb.at[1 - side], (t, mp)) for side, t in zip((far, 1 - far), to)], base
        )

    def layer_send(faces, members, zs, zr, base):
        blocks = [swap(faces(0, m, 2), faces(1, m, 2)) for m in range(members)]
        for m in range(0, members, 2):
            for side in range(2):
                value = blocks[m][side]
                if m + 1 < members:
                    other = roll(blocks[m + 1][side], 32 if side == 0 else -32)
                    value = jnp.where(flayer == (0 if side == 0 else L - 1), value, other)
                zs[side, :, FW * (m // 2) : FW * (m // 2 + 1)] = value
        remote([(zs.at[0], zr.at[1], (ms, below)), (zs.at[1], zr.at[0], (ms, above))], base)
        return blocks

    def plane_outside(own, rb, members, put, depth):
        lanes = lax.broadcasted_iota(jnp.int32, (1, members * FW), 1)
        member, node = lanes // FW, lax.rem(lanes, 32)
        row8 = lax.broadcasted_iota(jnp.int32, (8, 1), 0)
        rows = []
        for side in range(2):
            rows += [
                jnp.concatenate([rb[side, 4 * b + m] for m in range(4)], axis=1)
                for b in range(MAIN)
            ]
            if REM:
                parts = []
                for m in range(4):
                    part = jnp.zeros((8, FW), F32)
                    for e in range(REM):
                        to = REM * m + e
                        line = rb[side, 4 * MAIN + to // 8, to % 8 : to % 8 + 1, :]
                        part = jnp.where(row8 == e, line, part)
                    parts.append(part)
                rows.append(jnp.concatenate(parts, axis=1))
        received = jnp.concatenate(rows, axis=0)
        if members * FW > received.shape[1]:
            spare = jnp.zeros((2 * SP, FW), F32)
            for m in range(received.shape[1] // FW):
                part = roll(received[:, FW * m : FW * (m + 1)], 7 * m - 25)
                spare = jnp.where((fnode >= 7 * m) & (fnode < 7 * m + 7), part, spare)
            received = jnp.concatenate([received, spare], axis=1)
            pad = jnp.where(lax.rem(member, 4) == 0, 1.0, 0.0)
            received = jnp.where(node < 25, received, pad)
        got = own + choose(hot_recv, received, depth)
        for a in range(2):
            for m in range(members):
                lanes = slice(FW * m, FW * (m + 1))
                lo = got[a * C : (a + 1) * C, lanes]
                hi = got[(2 + a) * C : (3 + a) * C, lanes]
                primal, tangent = swap(lo, hi)
                put(0, m, a, primal)
                put(1, m, a, tangent)

    def layer_outside(blocks, zr, members, put):
        for m in range(members):
            lanes = slice(FW * (m // 2), FW * (m // 2 + 1))
            step = 32 * (L - 1 if m % 2 == 0 else L - 2)
            lo = jnp.where(flayer == 0, roll(zr[0, :, lanes], -step), roll(blocks[m][1], 32))
            hi = jnp.where(flayer == L - 1, roll(zr[1, :, lanes], step), roll(blocks[m][0], -32))
            primal, tangent = swap(lo, hi)
            put(0, m, 2, primal)
            put(1, m, 2, tangent)

    landed(xd, loads.at[0])
    for pt in range(2):
        for l in range(L):
            for m in range(5):
                pad = 1.0 if pt == 0 and m % 4 == 0 else 0.0
                u[pt, m, :, 128 * l + 120 : 128 * (l + 1)] = jnp.full((C, 8), pad, F32)
                u[pt, m, :, 128 * l : 128 * l + 125] = xd[pt, :, l, 125 * m : 125 * (m + 1)]
    for copy in inputs[2:6]:
        copy.wait()
    own_keys, recv_keys = key_ref[0:1, : 3 * OWN], key_ref[1:2, : 6 * SP]
    ri = lax.broadcasted_iota(jnp.int32, (SP, SLOTS), 0)
    li = lax.broadcasted_iota(jnp.int32, (SP, SLOTS), 1)
    send_hot = []
    for side in range(2):
        row = sr_ref[0, side : side + 1, :].astype(F32)
        wanted = jnp.sum(jnp.where(ri == li, row, 0.0), axis=1, keepdims=True)
        send_hot.append(jnp.where(wanted == own_keys, 1.0, 0.0))
    send_hot = jnp.concatenate(send_hot, axis=0).astype(BF16)

    def state_faces(a):
        for pt in range(2):
            for m in range(5):
                uf[pt, m, a] = trace(u[pt, m], a)

    state_faces(0)
    state_faces(1)
    table1 = plane_pack(lambda pt, m, a: uf[pt, m, a], 5, sb1)
    pl.semaphore_wait(barrier, len(greeted))
    plane_send(sb1, rb1, 0)
    if relayed:
        vouch(near, 0)
    state_faces(2)
    blocks1 = layer_send(lambda pt, m, a: uf[pt, m, a], 5, zs1, zr1, 1)

    source = [column(fs_ref[f : f + 1, :].astype(F32)) for f in range(4)]

    def hot(keys):
        rows = [jnp.where(source[2 * a + side] == keys, 1.0, 0.0) for side in range(2) for a in range(2)]
        return jnp.concatenate(rows, axis=0).astype(BF16)

    hot_own, hot_recv = hot(own_keys), hot(recv_keys)
    for a in range(3):
        wide = jnp.zeros((C, VW), F32)
        face = jnp.zeros((C, FW), F32)
        for l in range(L):
            value = column(metric_ref[a, l : l + 1, :])
            wide = jnp.where(vl // 128 == l, value, wide)
            face = jnp.where(flayer == l, value, face)
        mv[a] = wide
        mf[a] = face

    def gradients(rows):
        primal = [u[0, m, rows, :] for m in range(5)]
        tangent = [u[1, m, rows, :] for m in range(5)]
        fp, ft = jax.jvp(gradient_fields, (primal,), (tangent,))
        for m in range(4):
            w[0, m, rows, :] = fp[m]
            w[1, m, rows, :] = ft[m]

    blocks_of(gradients)
    inputs[6].wait()
    own1 = choose(hot_own, table1)
    fields = w[...].reshape(8 * C, VW)
    for a in range(3):
        q[a] = derive([a], [fields]).reshape(2, 4, C, VW)
    for a in range(3):
        for pt in range(2):
            for n, (b, f) in enumerate(needed(a)):
                qf[a, pt, n] = trace(q[b, pt, f], a)

    low_wall = jnp.where(source[2] < 0.0, 1.0, 0.0)
    high_wall = jnp.where(source[3] < 0.0, 1.0, 0.0)
    wall = jnp.where(first, low_wall, high_wall) > 0.5

    def put1(pt, m, a, value):
        if a == 1:
            own = uf[pt, m, a]
            value = jnp.where(wall, own if m % 4 == 0 else -own, value)
        of[pt, m, a] = value

    def face_fields(table, a, rows):
        primal = [table[0, m, a, rows, :] for m in range(5)]
        tangent = [table[1, m, a, rows, :] for m in range(5)]
        return jax.jvp(gradient_fields, (primal,), (tangent,))

    def insides(a):
        def body(rows):
            both = face_fields(uf, a, rows)
            for pt in range(2):
                for m in range(4):
                    jf[a, pt, m, rows, :] = both[pt][m]

        blocks_of(body)

    def jumps(a):
        def body(rows):
            both = face_fields(of, a, rows)
            for pt in range(2):
                for m in range(4):
                    jump = both[pt][m] - jf[a, pt, m, rows, :]
                    jf[a, pt, m, rows, :] = (0.5 * LIFT) * sign * jump

        blocks_of(body)

    for a in range(3):
        insides(a)

    def edge_jumps(a, b):
        there, lane = edges[a, b]
        for n, (other, f) in enumerate(needed(a)):
            if other == b:
                for pt in range(2):
                    qf[a, pt, n] += jnp.where(there, pull(jf[b, pt, f], lane), 0.0)

    arrived(zs1, zr1, 1)
    layer_outside(blocks1, zr1, 5, put1)
    jumps(2)
    edge_jumps(0, 2)
    edge_jumps(1, 2)
    arrived(sb1, rb1, 0)
    plane_outside(own1, rb1, 5, put1, 3)
    jumps(0)
    jumps(1)
    edge_jumps(0, 1)
    edge_jumps(1, 0)

    def face_viscous(a):
        def body(rows):
            states = [[uf[pt, m, a, rows, :] for m in range(5)] for pt in range(2)]
            grads = []
            for pt in range(2):
                grad = [[None] * 4 for _ in range(3)]
                for n, (b, f) in enumerate(needed(a)):
                    value = qf[a, pt, n, rows, :]
                    if b == a:
                        value = value + jf[a, pt, f, rows, :]
                    grad[b][f] = mf[b, rows, :] * value
                grads.append(grad)
            vp, vt = jax.jvp(
                lambda x, y: viscous_at(x, y, a), (states[0], grads[0]), (states[1], grads[1])
            )
            for m in range(4):
                vf[a, 0, m, rows, :] = vp[m]
                vf[a, 1, m, rows, :] = vt[m]

        blocks_of(body)

    face_viscous(0)
    face_viscous(1)
    table2 = plane_pack(lambda pt, m, a: vf[a, pt, m], 4, sb2)
    plane_send(sb2, rb2, 2)
    edge_jumps(2, 0)
    edge_jumps(2, 1)
    face_viscous(2)
    blocks2 = layer_send(lambda pt, m, a: vf[a, pt, m], 4, zs2, zr2, 3)

    own2 = choose(hot_own, table2)
    for a in range(3):
        q[a] += lift([a], [jf[a].reshape(8 * C, FW)]).reshape(2, 4, C, VW)

    def fluxes(rows):
        scale = [mv[a, rows, :] for a in range(3)]
        states = [[u[pt, m, rows, :] for m in range(5)] for pt in range(2)]
        grads = [
            [[scale[a] * q[a, pt, m, rows, :] for m in range(4)] for a in range(3)]
            for pt in range(2)
        ]
        visc = jax.jvp(viscous_all, (states[0], grads[0]), (states[1], grads[1]))
        for a in range(3):
            euler = jax.jvp(lambda x: inviscid(x, a), (states[0],), (states[1],))
            for pt in range(2):
                g[a, pt, 0, rows, :] = scale[a] * euler[pt][0]
                for m in range(4):
                    g[a, pt, m + 1, rows, :] = scale[a] * (euler[pt][m + 1] - visc[pt][a][m])

    blocks_of(fluxes)
    if relayed:
        vouched(near, 0)
        vouch(near[1:3], 4)
    for a in range(3):
        def surfaces(rows):
            primal = ([uf[0, m, a, rows, :] for m in range(5)], [of[0, m, a, rows, :] for m in range(5)])
            tangent = ([uf[1, m, a, rows, :] for m in range(5)], [of[1, m, a, rows, :] for m in range(5)])
            both = jax.jvp(
                lambda inner, outer: surface(inner, outer, sign, a), primal, tangent
            )
            scale = mf[a, rows, :]
            for pt in range(2):
                s[a, pt, 0, rows, :] = scale * both[pt][0]
                for m in range(4):
                    mine = (0.5 * LIFT) * sign * vf[a, pt, m, rows, :]
                    s[a, pt, m + 1, rows, :] = scale * (both[pt][m + 1] + mine)

        blocks_of(surfaces)

    total = derive(range(3), [g[a].reshape(10 * C, VW) for a in range(3)])
    total += lift(range(3), [s[a].reshape(10 * C, FW) for a in range(3)])
    r[...] = total.reshape(2, 5, C, VW)

    def whole_sum(parts):
        acc = parts[0]
        for part in parts[1:]:
            acc = acc + part
        return jnp.sum(jnp.sum(acc, axis=0, keepdims=True), axis=1, keepdims=True)

    pd = whole_sum([r[1, m] * u[1, m] for m in range(5)])
    dd = whole_sum([u[1, m] * u[1, m] for m in range(5)])
    mine = ratio(pd, dd)

    def put2(pt, m, a, value):
        if a == 1:
            value = jnp.where(wall, vf[a, pt, m], value)
        s[a, pt, m] = (-0.5 * LIFT) * sign * mf[a] * value

    arrived(zs2, zr2, 3)
    layer_outside(blocks2, zr2, 4, put2)

    arrived(sb2, rb2, 2)
    if relayed:
        vouched(near[1:3], 4)
    plane_outside(own2, rb2, 4, put2, 2)
    lifted = lift(range(3), [s[a, :, :4].reshape(8 * C, FW) for a in range(3)])
    lifted = lifted.reshape(2, 4, C, VW)
    for pt in range(2):
        r[pt, 1:] += lifted[pt]
    rests = [r[1, m] - mine * u[1, m] for m in range(5)]
    rs = whole_sum([r[0, m] * r[0, m] for m in range(5)])
    rr = whole_sum([x * x for x in rests])
    rd = whole_sum([x * u[1, m] for m, x in enumerate(rests)])
    lane = lax.broadcasted_iota(jnp.int32, (1, 128), 1)
    row = jnp.zeros((1, 128), F32)
    for i, value in enumerate((mine, dd, rs, rr, rd)):
        row = jnp.where(lane == i, value, row)
    st[...] = row
    for k in range(1, everyone):
        pltpu.make_async_remote_copy(
            src_ref=st, dst_ref=sta.at[k], send_sem=stsem.at[0], recv_sem=stsem.at[1],
            device_id=peer(k), device_id_type=MESH,
        ).start()
    sta[0] = st[...]
    own_ref[...] = xd[1]
    for pt, part in enumerate((res_ref, prod_ref)):
        for l in range(L):
            for m in range(5):
                part[:, l, 125 * m : 125 * (m + 1)] = r[pt, m, :, 128 * l : 128 * l + 125]
    landed(sta.at[pl.ds(1, everyone - 1)], stsem.at[1])
    landed(sta.at[pl.ds(1, everyone - 1)], stsem.at[0])
    table_ref[...] = sta[...].reshape(everyone, 128)


def finish(total_count, res, prod, d, table_ref, res_hbm, basis_hbm, kry_hbm, basis, kry, sems):
    first = pltpu.make_async_copy(res, res_hbm, sems.at[0])
    first.start()
    lane = lax.broadcasted_iota(jnp.int32, (1, 128), 1)
    table = table_ref[...]
    mine, dd, rs, rr, rd = [
        jnp.sum(jnp.where(lane == i, table, 0.0), axis=1, keepdims=True) for i in range(5)
    ]
    coefficient = jnp.sum(rd + mine * dd, axis=0, keepdims=True) * (1.0 / total_count)
    shift = mine - coefficient
    rr = jnp.sum(rr + 2.0 * shift * rd + shift * shift * dd, axis=0, keepdims=True)
    rs = jnp.sum(rs, axis=0, keepdims=True)
    beta = jnp.sqrt(rr * (1.0 / total_count))
    norm = jnp.sqrt(rs * (1.0 / total_count))
    row = jnp.where(lane == 0, coefficient, jnp.where(lane == 1, beta, norm))
    kry[...] = row[0, :3]
    third = pltpu.make_async_copy(kry, kry_hbm, sems.at[2])
    third.start()
    c, inv = coefficient, 1.0 / beta
    basis[...] = (prod[...] - c[:, :, None] * d[...]) * inv[:, :, None]
    second = pltpu.make_async_copy(basis, basis_hbm, sems.at[1])
    second.start()
    first.wait()
    third.wait()
    second.wait()


def local(ns, np_, state, direction, metric, face_source, send_rows):
    C, L, width = state.shape
    slots = send_rows.shape[2]
    SP = -(-slots // 8) * 8
    VW, FW = 128 * L, 64 * L
    own = 4 * C
    keys = np.full((2, max(3 * own, 6 * SP)), -7, np.float32)
    side, rest = np.divmod(np.arange(own), 2 * C)
    keys[0, : 3 * own] = np.tile(4 * (rest % C) + 2 * (rest // C) + side, 3)
    for copy in range(3):
        for side in range(2):
            at = (2 * copy + side) * SP
            keys[1, at : at + slots] = own + side * slots + np.arange(slots)
    tiles = 4 * (slots // 8) + -(-4 * (slots % 8) // 8)
    operands = (
        state, direction, jnp.transpose(metric, (2, 1, 0)), face_source.T, send_rows,
        jnp.asarray(keys), jnp.asarray(operators(L)),
    )
    operands = [pltpu.with_memory_space_constraint(x, pltpu.HBM) for x in operands]
    vmem = lambda *shape: pltpu.VMEM(shape, F32)
    dma = lambda n: pltpu.SemaphoreType.DMA((n,))
    spec = pl.BlockSpec(memory_space=pltpu.VMEM)
    parts, product, own, table = pl.pallas_call(
        functools.partial(kernel, ns, np_),
        out_shape=(
            *[jax.ShapeDtypeStruct(state.shape, F32)] * 3,
            jax.ShapeDtypeStruct((ns * np_, 128), F32),
        ),
        in_specs=[pl.BlockSpec(memory_space=pltpu.HBM)] * 7,
        out_specs=(spec,) * 4,
        scratch_shapes=[
            vmem(2, 5, C, VW), vmem(2, 5, 3, C, FW), vmem(2, 5, 3, C, FW),
            vmem(2, 4, C, VW), vmem(3, 2, 4, C, FW), vmem(3, 2, 4, C, VW),
            vmem(3, 2, 8, C, FW), vmem(3, 2, 4, C, FW),
            vmem(3, 2, 5, C, VW), vmem(3, 2, 5, C, FW), vmem(2, 5, C, VW),
            vmem(3, C, VW), vmem(3, C, FW),
            vmem(2, tiles, 8, FW), vmem(2, tiles, 8, FW), vmem(2, C, 3 * FW), vmem(2, C, 3 * FW),
            vmem(2, tiles, 8, FW), vmem(2, tiles, 8, FW), vmem(2, C, 2 * FW), vmem(2, C, 2 * FW),
            vmem(1, 128), vmem(ns * np_, 1, 128),
            vmem(2, C, L, width), *[pltpu.VMEM(x.shape, x.dtype) for x in operands[2:]],
            dma(4), dma(4), dma(2), dma(6), pltpu.SemaphoreType.REGULAR((6,)),
        ],
        compiler_params=pltpu.CompilerParams(
            collective_id=0, has_side_effects=True, vmem_limit_bytes=40 * 1024 * 1024
        ),
        name="navier",
    )(*operands)
    hbm = pl.BlockSpec(memory_space=pltpu.HBM)
    return pl.pallas_call(
        functools.partial(finish, float(state.size * ns * np_)),
        out_shape=(
            jax.ShapeDtypeStruct(state.shape, F32),
            jax.ShapeDtypeStruct(state.shape, F32),
            jax.ShapeDtypeStruct((3,), F32),
        ),
        in_specs=[spec] * 4,
        out_specs=(hbm, hbm, hbm),
        scratch_shapes=[vmem(C, L, width), vmem(3), dma(3)],
        compiler_params=pltpu.CompilerParams(vmem_limit_bytes=16 * 1024 * 1024),
        name="finish",
    )(parts, product, own, table)


def solution(mesh):
    return jax.shard_map(
        functools.partial(local, mesh.shape["stream"], mesh.shape["span"]),
        mesh=mesh,
        in_specs=(
            P("stream", "span", None),
            P("stream", "span", None),
            P("stream", "span", None),
            P("stream", None),
            P("stream", None, None),
        ),
        out_specs=(P("stream", "span", None), P("stream", "span", None), P()),
        check_vma=False,
    )
```

```python
import functools
import math

import jax
import jax.numpy as jnp
import numpy as np
from jax import lax
from jax.experimental import pallas as pl
from jax.experimental.pallas import tpu as pltpu
from jax.sharding import PartitionSpec as P

GAMMA = 1.4
VISC = 0.01
COND = VISC * GAMMA / ((GAMMA - 1.0) * 0.72)
LIFT = 10.0
MESH = pl.DeviceIdType.MESH
F32, BF16 = jnp.float32, jnp.bfloat16


def diff_table():
    spread = math.sqrt(3.0 / 7.0)
    points = np.array([-1.0, -spread, 0.0, spread, 1.0])
    weights = np.array(
        [np.prod([points[i] - points[j] for j in range(5) if j != i]) for i in range(5)]
    )
    matrix = np.zeros((5, 5))
    for i in range(5):
        for j in range(5):
            if i != j:
                matrix[i, j] = weights[i] / (weights[j] * (points[i] - points[j]))
        matrix[i, i] = np.sum([1.0 / (points[i] - points[j]) for j in range(5) if j != i])
    return matrix


def operators(layers):
    table = diff_table()
    eye = np.eye(5)
    kron = [
        np.einsum("ai,bj,ck->ijkabc", *[table if m == a else eye for m in range(3)]).reshape(125, 125)
        for a in range(3)
    ]
    node = np.arange(125).reshape(5, 5, 5)
    vw, fw, half = 128 * layers, 64 * layers, 32 * layers
    deriv = np.zeros((3, vw, vw), np.float32)
    pick = np.zeros((3, vw, fw), np.float32)
    for a in range(3):
        for l in range(layers):
            b = 128 * l
            deriv[a, b : b + 125, b : b + 125] = kron[a]
            for side in range(2):
                face = np.take(node, 4 * side, axis=a).reshape(-1)
                for m, at in enumerate(face):
                    pick[a, b + at, side * half + 32 * l + m] = 1.0
    high = deriv.astype(jnp.bfloat16)
    low = (deriv - high.astype(np.float32)).astype(jnp.bfloat16)
    lift = np.swapaxes(pick, 1, 2).astype(jnp.bfloat16)
    return np.concatenate([low, high, lift], axis=1)


def pieces(x, n):
    out = []
    for i in range(n):
        p = x.astype(BF16)
        out.append(p)
        if i + 1 < n:
            x = x - p.astype(F32)
    return out


def dot(a, b):
    return jnp.dot(a, b, preferred_element_type=F32)


def fields_of(u):
    inv = 1.0 / u[0]
    vel = [u[1] * inv, u[2] * inv, u[3] * inv]
    kinetic = 0.5 * (u[1] * vel[0] + u[2] * vel[1] + u[3] * vel[2])
    pressure = (GAMMA - 1.0) * (u[4] - kinetic)
    return vel, pressure, pressure * inv


def inviscid(u, a):
    vel, pressure, _ = fields_of(u)
    out = [u[1 + a]]
    for m in range(3):
        term = u[1 + m] * vel[a]
        out.append(term + pressure if m == a else term)
    out.append((u[4] + pressure) * vel[a])
    return out


def viscous(vel, q, a, divergence):
    stress = []
    for m in range(3):
        term = q[a][m] + q[m][a]
        if m == a:
            term = term - 2.0 / 3.0 * divergence
        stress.append(VISC * term)
    energy = stress[0] * vel[0] + stress[1] * vel[1] + stress[2] * vel[2] + COND * q[a][3]
    return stress + [energy]


def viscous_all(u, q):
    inv = 1.0 / u[0]
    vel = [u[1] * inv, u[2] * inv, u[3] * inv]
    divergence = q[0][0] + q[1][1] + q[2][2]
    return [viscous(vel, q, a, divergence) for a in range(3)]


def viscous_at(u, q, a):
    inv = 1.0 / u[0]
    vel = [u[1] * inv, u[2] * inv, u[3] * inv]
    return viscous(vel, q, a, q[0][0] + q[1][1] + q[2][2])


def gradient_fields(u):
    vel, _, temper = fields_of(u)
    return vel + [temper]


def surface(inner, outer, sign, a):
    vi, pi, ti = fields_of(inner)
    vo, po, to = fields_of(outer)
    square = sum(v * v for v in vi) + GAMMA * ti + sum(v * v for v in vo) + GAMMA * to
    speed = jnp.sqrt(0.5 * square)
    fi, fo = inviscid(inner, a), inviscid(outer, a)
    return [
        (0.5 * LIFT) * (sign * (fo[m] - fi[m]) - speed * (outer[m] - inner[m])) for m in range(5)
    ]


def ratio(top, bottom):
    return jnp.where(bottom > 0.0, top / jnp.where(bottom > 0.0, bottom, 1.0), 0.0)


def needed(a):
    return [(a, f) for f in range(4)] + [x for b in range(3) if b != a for x in ((b, a), (b, b))]


def kernel(
    ns, np_,
    x_hbm, d_hbm, metric_hbm, fs_hbm, sr_hbm, key_hbm, ops_hbm,
    res_ref, prod_ref, own_ref, table_ref,
    u, uf, of, w, jf, q, qf, vf, ov, g, s, r, mv, mf, mj,
    sb1, rb1, zs1, zr1, sb2, rb2, zs2, zr2, st, sta,
    xd, metric_ref, fs_ref, sr_ref, key_ref, ops_ref,
    xsend, xrecv, stsem, loads, word,
):
    C, L = xd.shape[1], xd.shape[2]
    VW, FW, half = 128 * L, 64 * L, 32 * L
    SLOTS = sr_ref.shape[2]
    SP = -(-SLOTS // 8) * 8
    MAIN, REM = SLOTS // 8, SLOTS % 8
    OWN = 4 * C
    ms, mp = lax.axis_index("stream"), lax.axis_index("span")
    lower, upper = lax.rem(ms + ns - 1, ns), lax.rem(ms + 1, ns)
    below, above = lax.rem(mp + np_ - 1, np_), lax.rem(mp + 1, np_)

    inputs = [
        pltpu.make_async_copy(src, dst, loads.at[i])
        for src, dst, i in [
            (x_hbm, xd.at[0], 0), (d_hbm, xd.at[1], 0), (key_hbm, key_ref, 1), (fs_hbm, fs_ref, 2),
            (sr_hbm, sr_ref, 3), (metric_hbm, metric_ref, 4), (ops_hbm, ops_ref, 5),
        ]
    ]
    for copy in inputs:
        copy.start()

    def peer(k):
        a, b = divmod(k, np_)
        return lax.rem(ms + a, ns), lax.rem(mp + b, np_)

    everyone = ns * np_
    relayed = ns == 8
    near = [a * np_ for a in (1, 2, ns - 2, ns - 1)]
    greeted = near + list(range(1, np_)) if relayed else list(range(1, everyone))
    barrier = pltpu.get_barrier_semaphore()
    for k in greeted:
        pl.semaphore_signal(barrier, inc=1, device_id=peer(k), device_id_type=MESH)

    def vouch(which, i):
        for k in which:
            pl.semaphore_signal(word.at[i], inc=1, device_id=peer(k), device_id_type=MESH)

    def vouched(which, i):
        pl.semaphore_wait(word.at[i], len(which))

    fl = lax.broadcasted_iota(jnp.int32, (1, FW), 1)
    vl = lax.broadcasted_iota(jnp.int32, (1, VW), 1)
    first = fl < half
    sign = jnp.where(first, -1.0, 1.0)
    flayer = lax.rem(fl, half) // 32
    fnode = lax.rem(fl, 32)
    fside = jnp.where(first, 0, 1)
    major, minor = fnode // 5, lax.rem(fnode, 5)
    nodes = [
        jnp.where(fnode < 25, at, 127)
        for at in (100 * fside + fnode, 25 * major + 20 * fside + minor, 5 * fnode + 4 * fside)
    ]

    def pull(x, at):
        return jnp.take_along_axis(
            x, jnp.broadcast_to(at, x.shape), axis=1, mode="promise_in_bounds"
        )

    def trace(volume, a):
        value = None
        for l in range(L):
            part = pull(volume[:, 128 * l : 128 * (l + 1)], nodes[a])
            value = part if value is None else jnp.where(flayer == l, part, value)
        return value

    def edge(a, b):
        at = dict(zip([x for x in range(3) if x != a], (major, minor)))
        at[a] = 4 * fside
        one, two = [x for x in range(3) if x != b]
        there = (lax.rem(at[b], 4) == 0) & (fnode < 25)
        lane = half * (at[b] // 4) + 32 * flayer + 5 * at[one] + at[two]
        return there, jnp.where(there, lane, 0)

    edges = {(a, b): edge(a, b) for a in range(3) for b in range(3) if a != b}

    def roll(x, shift):
        shift = shift % FW
        return pltpu.roll(x, shift, 1) if shift else x

    di = lax.broadcasted_iota(jnp.int32, (C, C), 0)
    dj = lax.broadcasted_iota(jnp.int32, (C, C), 1)

    def column(row):
        return jnp.sum(jnp.where(di == dj, row, 0.0), axis=1, keepdims=True)

    def blocks_of(body):
        @pl.loop(0, C // 8, unroll=True)
        def _(i):
            body(pl.ds(pl.multiple_of(i * 8, 8), 8))

    def lift(axes, values):
        halves, table = [], []
        for a, value in zip(axes, values):
            halves += pieces(value, 2)
            table += [ops_ref[a, 2 * VW :]] * 2
        return dot(jnp.concatenate(halves, axis=1), jnp.concatenate(table, axis=0))

    def derive(axes, values):
        halves, table = [], []
        for a, value in zip(axes, values):
            high, low = pieces(value, 2)
            halves += [high, low, high]
            table += [ops_ref[a, : 2 * VW], ops_ref[a, VW : 2 * VW]]
        return dot(jnp.concatenate(halves, axis=1), jnp.concatenate(table, axis=0))

    def choose(hot, x, depth=3):
        return dot(hot[:, : depth * x.shape[0]], jnp.concatenate(pieces(x, depth)[::-1], axis=0))

    def swap(a, b):
        return (
            jnp.where(first, a, pltpu.roll(b, half, 1)),
            jnp.where(first, pltpu.roll(a, half, 1), b),
        )

    def landed(ref, sem):
        pltpu.make_async_copy(ref, ref, sem).wait()

    def remote(pairs, base):
        for src, dst, to in pairs:
            pltpu.make_async_remote_copy(
                src_ref=src, dst_ref=dst, send_sem=xsend.at[base],
                recv_sem=xrecv.at[base], device_id=to, device_id_type=MESH,
            ).start()

    def arrived(source, target, base):
        landed(target, xrecv.at[base])
        landed(source, xsend.at[base])

    def plane_pack(faces, members, sb):
        blocks = [[swap(faces(0, m, a), faces(1, m, a)) for m in members] for a in range(2)]
        table = jnp.concatenate(
            [
                jnp.concatenate([blocks[a][m][side] for m in range(len(members))], axis=1)
                for side in range(2)
                for a in range(2)
            ],
            axis=0,
        )
        sent = choose(send_hot, table)
        for i, m in enumerate(members[:4]):
            value = sent[:, FW * i : FW * (i + 1)]
            if len(members) > 4:
                spare = roll(sent[:, 4 * FW :], 25 - 7 * m)
                value = jnp.where(fnode < 25, value, spare)
            for side in range(2):
                for b in range(MAIN):
                    at = side * SP + 8 * b
                    sb[side, MAIN * m + b] = value[at : at + 8]
                for e in range(REM):
                    at, to = side * SP + 8 * MAIN + e, REM * m + e
                    sb[side, 4 * MAIN + to // 8, to % 8 : to % 8 + 1, :] = value[at : at + 1]
        return table

    def plane_send(sb, rb, base, part=slice(None)):
        far = lax.rem(ms, 2)
        to = [lax.rem(ms + ns - 1 + 2 * side, ns) for side in (far, 1 - far)]
        remote(
            [
                (sb.at[side, part], rb.at[1 - side, part], (t, mp))
                for side, t in zip((far, 1 - far), to)
            ],
            base,
        )

    def layer_send(faces, members, zs, zr, base):
        blocks = [swap(faces(0, m, 2), faces(1, m, 2)) for m in range(members)]
        for m in range(0, members, 2):
            for side in range(2):
                value = blocks[m][side]
                if m + 1 < members:
                    other = roll(blocks[m + 1][side], 32 if side == 0 else -32)
                    value = jnp.where(flayer == (0 if side == 0 else L - 1), value, other)
                zs[side, :, FW * (m // 2) : FW * (m // 2 + 1)] = value
        remote([(zs.at[0], zr.at[1], (ms, below)), (zs.at[1], zr.at[0], (ms, above))], base)
        return blocks

    def plane_outside(own, rb, members, put, depth):
        lanes = lax.broadcasted_iota(jnp.int32, (1, members * FW), 1)
        member, node = lanes // FW, lax.rem(lanes, 32)
        row8 = lax.broadcasted_iota(jnp.int32, (8, 1), 0)
        rows = []
        for side in range(2):
            rows += [
                jnp.concatenate([rb[side, MAIN * m + b] for m in range(4)], axis=1)
                for b in range(MAIN)
            ]
            if REM:
                parts = []
                for m in range(4):
                    part = jnp.zeros((8, FW), F32)
                    for e in range(REM):
                        to = REM * m + e
                        line = rb[side, 4 * MAIN + to // 8, to % 8 : to % 8 + 1, :]
                        part = jnp.where(row8 == e, line, part)
                    parts.append(part)
                rows.append(jnp.concatenate(parts, axis=1))
        received = jnp.concatenate(rows, axis=0)
        if members * FW > received.shape[1]:
            spare = jnp.zeros((2 * SP, FW), F32)
            for m in range(received.shape[1] // FW):
                part = roll(received[:, FW * m : FW * (m + 1)], 7 * m - 25)
                spare = jnp.where((fnode >= 7 * m) & (fnode < 7 * m + 7), part, spare)
            received = jnp.concatenate([received, spare], axis=1)
            pad = jnp.where(lax.rem(member, 4) == 0, 1.0, 0.0)
            received = jnp.where(node < 25, received, pad)
        got = choose(hot_recv, received, depth)
        spread(got if own is None else own + got, members, put)

    def spread(got, members, put):
        for a in range(2):
            for m in range(members):
                lanes = slice(FW * m, FW * (m + 1))
                lo = got[a * C : (a + 1) * C, lanes]
                hi = got[(2 + a) * C : (3 + a) * C, lanes]
                primal, tangent = swap(lo, hi)
                put(0, m, a, primal)
                put(1, m, a, tangent)

    def layer_outside(blocks, zr, members, put):
        for m in range(members):
            lanes = slice(FW * (m // 2), FW * (m // 2 + 1))
            step = 32 * (L - 1 if m % 2 == 0 else L - 2)
            lo = jnp.where(flayer == 0, roll(zr[0, :, lanes], -step), roll(blocks[m][1], 32))
            hi = jnp.where(flayer == L - 1, roll(zr[1, :, lanes], step), roll(blocks[m][0], -32))
            primal, tangent = swap(lo, hi)
            put(0, m, 2, primal)
            put(1, m, 2, tangent)

    landed(xd, loads.at[0])
    for pt in range(2):
        for l in range(L):
            for m in range(5):
                pad = 1.0 if pt == 0 and m % 4 == 0 else 0.0
                u[pt, m, :, 128 * l + 120 : 128 * (l + 1)] = jnp.full((C, 8), pad, F32)
                u[pt, m, :, 128 * l : 128 * l + 125] = xd[pt, :, l, 125 * m : 125 * (m + 1)]
    for copy in inputs[2:6]:
        copy.wait()
    own_keys, recv_keys = key_ref[0:1, : 3 * OWN], key_ref[1:2, : 6 * SP]
    ri = lax.broadcasted_iota(jnp.int32, (SP, SLOTS), 0)
    li = lax.broadcasted_iota(jnp.int32, (SP, SLOTS), 1)
    send_hot = []
    for side in range(2):
        row = sr_ref[0, side : side + 1, :].astype(F32)
        wanted = jnp.sum(jnp.where(ri == li, row, 0.0), axis=1, keepdims=True)
        send_hot.append(jnp.where(wanted == own_keys, 1.0, 0.0))
    send_hot = jnp.concatenate(send_hot, axis=0).astype(BF16)

    def state_faces(a):
        for pt in range(2):
            for m in range(5):
                uf[pt, m, a] = trace(u[pt, m], a)

    state_faces(0)
    state_faces(1)
    table1 = plane_pack(lambda pt, m, a: uf[pt, m, a], range(5), sb1)
    pl.semaphore_wait(barrier, len(greeted))
    plane_send(sb1, rb1, 0)
    if relayed:
        vouch(near, 0)
    state_faces(2)
    blocks1 = layer_send(lambda pt, m, a: uf[pt, m, a], 5, zs1, zr1, 1)

    source = [column(fs_ref[f : f + 1, :].astype(F32)) for f in range(4)]

    def hot(keys):
        rows = [jnp.where(source[2 * a + side] == keys, 1.0, 0.0) for side in range(2) for a in range(2)]
        return jnp.concatenate(rows, axis=0).astype(BF16)

    hot_own, hot_recv = hot(own_keys), hot(recv_keys)
    for a in range(3):
        wide = jnp.zeros((C, VW), F32)
        face = jnp.zeros((C, FW), F32)
        for l in range(L):
            value = column(metric_ref[a, l : l + 1, :])
            wide = jnp.where(vl // 128 == l, value, wide)
            face = jnp.where(flayer == l, value, face)
        mv[a] = wide
        mf[a] = face
        mj[a] = (-0.5 * LIFT) * sign * face

    def gradients(rows):
        primal = [u[0, m, rows, :] for m in range(5)]
        tangent = [u[1, m, rows, :] for m in range(5)]
        fp, ft = jax.jvp(gradient_fields, (primal,), (tangent,))
        for m in range(4):
            w[0, m, rows, :] = fp[m]
            w[1, m, rows, :] = ft[m]

    blocks_of(gradients)
    inputs[6].wait()
    own1 = choose(hot_own, table1)
    fields = w[...].reshape(8 * C, VW)
    for a in range(3):
        q[a] = derive([a], [fields]).reshape(2, 4, C, VW)
    for a in range(3):
        for pt in range(2):
            for n, (b, f) in enumerate(needed(a)):
                qf[a, pt, n] = trace(q[b, pt, f], a)

    low_wall = jnp.where(source[2] < 0.0, 1.0, 0.0)
    high_wall = jnp.where(source[3] < 0.0, 1.0, 0.0)
    wall = jnp.where(first, low_wall, high_wall) > 0.5

    def put1(pt, m, a, value):
        if a == 1:
            own = uf[pt, m, a]
            value = jnp.where(wall, own if m % 4 == 0 else -own, value)
        of[pt, m, a] = value

    def face_fields(table, a, rows):
        primal = [table[0, m, a, rows, :] for m in range(5)]
        tangent = [table[1, m, a, rows, :] for m in range(5)]
        return jax.jvp(gradient_fields, (primal,), (tangent,))

    def insides(a):
        def body(rows):
            both = face_fields(uf, a, rows)
            for pt in range(2):
                for m in range(4):
                    jf[a, pt, m, rows, :] = both[pt][m]

        blocks_of(body)

    def jumps(a):
        def body(rows):
            both = face_fields(of, a, rows)
            for pt in range(2):
                for m in range(4):
                    jump = both[pt][m] - jf[a, pt, m, rows, :]
                    jf[a, pt, m, rows, :] = (0.5 * LIFT) * sign * jump

        blocks_of(body)

    for a in range(3):
        insides(a)

    def edge_jumps(a, b):
        there, lane = edges[a, b]
        for n, (other, f) in enumerate(needed(a)):
            if other == b:
                for pt in range(2):
                    qf[a, pt, n] += jnp.where(there, pull(jf[b, pt, f], lane), 0.0)

    arrived(zs1, zr1, 1)
    layer_outside(blocks1, zr1, 5, put1)
    jumps(2)
    edge_jumps(0, 2)
    edge_jumps(1, 2)
    arrived(sb1, rb1, 0)
    plane_outside(own1, rb1, 5, put1, 3)
    jumps(0)
    jumps(1)
    edge_jumps(0, 1)
    edge_jumps(1, 0)

    def face_viscous(a):
        def body(rows):
            states = [[uf[pt, m, a, rows, :] for m in range(5)] for pt in range(2)]
            grads = []
            for pt in range(2):
                grad = [[None] * 4 for _ in range(3)]
                for n, (b, f) in enumerate(needed(a)):
                    value = qf[a, pt, n, rows, :]
                    if b == a:
                        value = value + jf[a, pt, f, rows, :]
                    grad[b][f] = mf[b, rows, :] * value
                grads.append(grad)
            vp, vt = jax.jvp(
                lambda x, y: viscous_at(x, y, a), (states[0], grads[0]), (states[1], grads[1])
            )
            for m in range(4):
                vf[a, 0, m, rows, :] = vp[m]
                vf[a, 1, m, rows, :] = vt[m]

        blocks_of(body)

    face_viscous(0)
    face_viscous(1)
    table2 = []
    for some in (range(0, 2), range(2, 4)):
        table2.append(plane_pack(lambda pt, m, a: vf[a, pt, m], some, sb2))
        ends = [MAIN * some[0], MAIN * (some[-1] + 1) if some[-1] < 3 else sb2.shape[1]]
        plane_send(sb2, rb2, 2, pl.ds(ends[0], ends[1] - ends[0]))
    edge_jumps(2, 0)
    edge_jumps(2, 1)
    face_viscous(2)
    blocks2 = layer_send(lambda pt, m, a: vf[a, pt, m], 4, zs2, zr2, 3)


    def put_own(pt, m, a, value):
        ov[a, pt, m] = jnp.where(wall, vf[a, pt, m], value) if a == 1 else value

    spread(choose(hot_own, jnp.concatenate(table2, axis=1)), 4, put_own)
    for a in range(3):
        q[a] += lift([a], [jf[a].reshape(8 * C, FW)]).reshape(2, 4, C, VW)

    def fluxes(rows):
        scale = [mv[a, rows, :] for a in range(3)]
        states = [[u[pt, m, rows, :] for m in range(5)] for pt in range(2)]
        grads = [
            [[scale[a] * q[a, pt, m, rows, :] for m in range(4)] for a in range(3)]
            for pt in range(2)
        ]
        visc = jax.jvp(viscous_all, (states[0], grads[0]), (states[1], grads[1]))
        for a in range(3):
            euler = jax.jvp(lambda x: inviscid(x, a), (states[0],), (states[1],))
            for pt in range(2):
                g[a, pt, 0, rows, :] = scale[a] * euler[pt][0]
                for m in range(4):
                    g[a, pt, m + 1, rows, :] = scale[a] * (euler[pt][m + 1] - visc[pt][a][m])

    blocks_of(fluxes)
    if relayed:
        vouched(near, 0)
        vouch(near[1:3], 1)
    for a in range(3):
        def surfaces(rows):
            primal = ([uf[0, m, a, rows, :] for m in range(5)], [of[0, m, a, rows, :] for m in range(5)])
            tangent = ([uf[1, m, a, rows, :] for m in range(5)], [of[1, m, a, rows, :] for m in range(5)])
            both = jax.jvp(
                lambda inner, outer: surface(inner, outer, sign, a), primal, tangent
            )
            scale = mf[a, rows, :]
            for pt in range(2):
                s[a, pt, 0, rows, :] = scale * both[pt][0]
                for m in range(4):
                    inner = vf[a, pt, m, rows, :]
                    if a < 2:
                        inner = inner - ov[a, pt, m, rows, :]
                    s[a, pt, m + 1, rows, :] = scale * both[pt][m + 1] - mj[a, rows, :] * inner

        blocks_of(surfaces)

    total = derive(range(3), [g[a].reshape(10 * C, VW) for a in range(3)])
    total += lift(range(3), [s[a].reshape(10 * C, FW) for a in range(3)])
    r[...] = total.reshape(2, 5, C, VW)

    def whole_sum(parts):
        acc = parts[0]
        for part in parts[1:]:
            acc = acc + part
        return jnp.sum(jnp.sum(acc, axis=0, keepdims=True), axis=1, keepdims=True)

    pd = whole_sum([r[1, m] * u[1, m] for m in range(5)])
    dd = whole_sum([u[1, m] * u[1, m] for m in range(5)])
    mine = ratio(pd, dd)

    def put2(pt, m, a, value):
        s[a, pt, m] = mj[a] * value

    arrived(zs2, zr2, 3)
    layer_outside(blocks2, zr2, 4, put2)

    arrived(sb2, rb2, 2)
    if relayed:
        vouched(near[1:3], 1)
    plane_outside(None, rb2, 4, put2, 2)
    lifted = lift(range(3), [s[a, :, :4].reshape(8 * C, FW) for a in range(3)])
    lifted = lifted.reshape(2, 4, C, VW)
    for pt in range(2):
        r[pt, 1:] += lifted[pt]
    rests = [r[1, m] - mine * u[1, m] for m in range(5)]
    rs = whole_sum([r[0, m] * r[0, m] for m in range(5)])
    rr = whole_sum([x * x for x in rests])
    rd = whole_sum([x * u[1, m] for m, x in enumerate(rests)])
    lane = lax.broadcasted_iota(jnp.int32, (1, 128), 1)
    row = jnp.zeros((1, 128), F32)
    for i, value in enumerate((mine, dd, rs, rr, rd)):
        row = jnp.where(lane == i, value, row)
    st[...] = row
    for k in range(1, everyone):
        pltpu.make_async_remote_copy(
            src_ref=st, dst_ref=sta.at[k], send_sem=stsem.at[0], recv_sem=stsem.at[1],
            device_id=peer(k), device_id_type=MESH,
        ).start()
    sta[0] = st[...]
    own_ref[...] = xd[1]
    for pt, part in enumerate((res_ref, prod_ref)):
        for l in range(L):
            for m in range(5):
                part[:, l, 125 * m : 125 * (m + 1)] = r[pt, m, :, 128 * l : 128 * l + 125]
    landed(sta.at[pl.ds(1, everyone - 1)], stsem.at[1])
    landed(sta.at[pl.ds(1, everyone - 1)], stsem.at[0])
    table_ref[...] = sta[...].reshape(everyone, 128)


def finish(total_count, res, prod, d, table_ref, res_hbm, basis_hbm, kry_hbm, basis, kry, sems):
    first = pltpu.make_async_copy(res, res_hbm, sems.at[0])
    first.start()
    lane = lax.broadcasted_iota(jnp.int32, (1, 128), 1)
    table = table_ref[...]
    mine, dd, rs, rr, rd = [
        jnp.sum(jnp.where(lane == i, table, 0.0), axis=1, keepdims=True) for i in range(5)
    ]
    coefficient = jnp.sum(rd + mine * dd, axis=0, keepdims=True) * (1.0 / total_count)
    shift = mine - coefficient
    rr = jnp.sum(rr + 2.0 * shift * rd + shift * shift * dd, axis=0, keepdims=True)
    rs = jnp.sum(rs, axis=0, keepdims=True)
    beta = jnp.sqrt(rr * (1.0 / total_count))
    norm = jnp.sqrt(rs * (1.0 / total_count))
    row = jnp.where(lane == 0, coefficient, jnp.where(lane == 1, beta, norm))
    kry[...] = row[0, :3]
    third = pltpu.make_async_copy(kry, kry_hbm, sems.at[2])
    third.start()
    c, inv = coefficient, 1.0 / beta
    basis[...] = (prod[...] - c[:, :, None] * d[...]) * inv[:, :, None]
    second = pltpu.make_async_copy(basis, basis_hbm, sems.at[1])
    second.start()
    first.wait()
    third.wait()
    second.wait()


def local(ns, np_, state, direction, metric, face_source, send_rows):
    C, L, width = state.shape
    slots = send_rows.shape[2]
    SP = -(-slots // 8) * 8
    VW, FW = 128 * L, 64 * L
    own = 4 * C
    keys = np.full((2, max(3 * own, 6 * SP)), -7, np.float32)
    side, rest = np.divmod(np.arange(own), 2 * C)
    keys[0, : 3 * own] = np.tile(4 * (rest % C) + 2 * (rest // C) + side, 3)
    for copy in range(3):
        for side in range(2):
            at = (2 * copy + side) * SP
            keys[1, at : at + slots] = own + side * slots + np.arange(slots)
    tiles = 4 * (slots // 8) + -(-4 * (slots % 8) // 8)
    operands = (
        state, direction, jnp.transpose(metric, (2, 1, 0)), face_source.T, send_rows,
        jnp.asarray(keys), jnp.asarray(operators(L)),
    )
    operands = [pltpu.with_memory_space_constraint(x, pltpu.HBM) for x in operands]
    vmem = lambda *shape: pltpu.VMEM(shape, F32)
    dma = lambda n: pltpu.SemaphoreType.DMA((n,))
    spec = pl.BlockSpec(memory_space=pltpu.VMEM)
    parts, product, own, table = pl.pallas_call(
        functools.partial(kernel, ns, np_),
        out_shape=(
            *[jax.ShapeDtypeStruct(state.shape, F32)] * 3,
            jax.ShapeDtypeStruct((ns * np_, 128), F32),
        ),
        in_specs=[pl.BlockSpec(memory_space=pltpu.HBM)] * 7,
        out_specs=(spec,) * 4,
        scratch_shapes=[
            vmem(2, 5, C, VW), vmem(2, 5, 3, C, FW), vmem(2, 5, 3, C, FW),
            vmem(2, 4, C, VW), vmem(3, 2, 4, C, FW), vmem(3, 2, 4, C, VW),
            vmem(3, 2, 8, C, FW), vmem(3, 2, 4, C, FW), vmem(2, 2, 4, C, FW),
            vmem(3, 2, 5, C, VW), vmem(3, 2, 5, C, FW), vmem(2, 5, C, VW),
            vmem(3, C, VW), vmem(3, C, FW), vmem(3, C, FW),
            vmem(2, tiles, 8, FW), vmem(2, tiles, 8, FW), vmem(2, C, 3 * FW), vmem(2, C, 3 * FW),
            vmem(2, tiles, 8, FW), vmem(2, tiles, 8, FW), vmem(2, C, 2 * FW), vmem(2, C, 2 * FW),
            vmem(1, 128), vmem(ns * np_, 1, 128),
            vmem(2, C, L, width), *[pltpu.VMEM(x.shape, x.dtype) for x in operands[2:]],
            dma(4), dma(4), dma(2), dma(6), pltpu.SemaphoreType.REGULAR((2,)),
        ],
        compiler_params=pltpu.CompilerParams(
            collective_id=0, has_side_effects=True, vmem_limit_bytes=40 * 1024 * 1024
        ),
        name="navier",
    )(*operands)
    hbm = pl.BlockSpec(memory_space=pltpu.HBM)
    return pl.pallas_call(
        functools.partial(finish, float(state.size * ns * np_)),
        out_shape=(
            jax.ShapeDtypeStruct(state.shape, F32),
            jax.ShapeDtypeStruct(state.shape, F32),
            jax.ShapeDtypeStruct((3,), F32),
        ),
        in_specs=[spec] * 4,
        out_specs=(hbm, hbm, hbm),
        scratch_shapes=[vmem(C, L, width), vmem(3), dma(3)],
        compiler_params=pltpu.CompilerParams(vmem_limit_bytes=16 * 1024 * 1024),
        name="finish",
    )(parts, product, own, table)


def solution(mesh):
    return jax.shard_map(
        functools.partial(local, mesh.shape["stream"], mesh.shape["span"]),
        mesh=mesh,
        in_specs=(
            P("stream", "span", None),
            P("stream", "span", None),
            P("stream", "span", None),
            P("stream", None),
            P("stream", None, None),
        ),
        out_specs=(P("stream", "span", None), P("stream", "span", None), P()),
        check_vma=False,
    )
```
